8 devices in a mesh: replica: 1 (over z), heads: 2 (over y), model: 4 (over x, core).
Axes of the slice: x: 2, y: 2, z: 1, core: 2. Of those that a mesh axis runs over, the one named last changes fastest.
Arguments:
- tokens: bfloat16 [128, 18432], P('replica')
- w_query: bfloat16 [18432, 12288], P(None, ('heads', 'model'))
- w_key: bfloat16 [18432, 256], replicated
- w_value: bfloat16 [18432, 256], replicated
- w_out: bfloat16 [12288, 18432], P(('heads', 'model'))
- key_cache: bfloat16 [128, 1, 4096, 256], P(('replica', 'model'))
- value_cache: bfloat16 [128, 1, 4096, 256], P(('replica', 'model'))
- lengths: int32 [128], P(('replica', 'model'))
Outputs:
- output 1: bfloat16 [128, 18432], P('replica')
- output 2: bfloat16 [128, 1, 256], P(('replica', 'model'))
- output 3: bfloat16 [128, 1, 256], P(('replica', 'model'))
All inputs are finite; a program needn't handle non-finite values.
Results may differ from the reference program's by a relative error of at most 0.00214.
Values are sent between devices in bfloat16 or wider.
A program may use at most 1.25 GiB of HBM per device.

```python
import jax
import jax.numpy as jnp
from jax import lax

D = 18432
QHEADS = 48
KVHEADS = 1
HEAD = 256
BATCH = 128
CONTEXT = 4096
GROUP_SIZE = QHEADS // KVHEADS
SCALE = HEAD ** -0.5


def draw_lengths(len_key):
    len_keys = jax.random.split(len_key, 2)
    lengths = jax.random.randint(len_keys[0], (BATCH,), 1, CONTEXT, dtype=jnp.int32)
    perm_order = jax.random.permutation(len_keys[1], BATCH)
    return lengths.at[perm_order[0]].set(CONTEXT - 1).at[perm_order[1]].set(1)


def setup_inputs(seed: int = 0, part: int = 0) -> dict:
    base_key = jax.random.key(seed)
    part_key = jax.random.fold_in(base_key, part)
    part_keys = jax.random.split(part_key, 3)
    weight_keys = jax.random.split(base_key, 4)
    query_cols = QHEADS * HEAD
    kv_cols = KVHEADS * HEAD
    tokens = jax.random.normal(part_keys[0], (BATCH, D), jnp.float32)
    w_query = jax.random.normal(weight_keys[0], (D, query_cols), jnp.float32) * D ** -0.5
    w_key = jax.random.normal(weight_keys[1], (D, kv_cols), jnp.float32) * (3.0 * D ** -0.5)
    w_value = jax.random.normal(weight_keys[2], (D, kv_cols), jnp.float32) * D ** -0.5
    w_out = jax.random.normal(weight_keys[3], (query_cols, D), jnp.float32) * query_cols ** -0.5
    key_cache = 3.0 * jax.random.normal(part_keys[1], (BATCH, KVHEADS, CONTEXT, HEAD), jnp.float32)
    value_cache = jax.random.normal(part_keys[2], (BATCH, KVHEADS, CONTEXT, HEAD), jnp.float32)
    lengths = draw_lengths(jax.random.fold_in(part_key, 3))
    return {
        "tokens": tokens.astype(jnp.bfloat16),
        "w_query": w_query.astype(jnp.bfloat16),
        "w_key": w_key.astype(jnp.bfloat16),
        "w_value": w_value.astype(jnp.bfloat16),
        "w_out": w_out.astype(jnp.bfloat16),
        "key_cache": key_cache.astype(jnp.bfloat16),
        "value_cache": value_cache.astype(jnp.bfloat16),
        "lengths": lengths,
    }


def reference(tokens, w_query, w_key, w_value, w_out, key_cache, value_cache, lengths):
    queries = jnp.dot(tokens, w_query, preferred_element_type=jnp.float32).astype(jnp.bfloat16)
    queries = queries.reshape(BATCH, KVHEADS, GROUP_SIZE, HEAD)
    key_new = jnp.dot(tokens, w_key, preferred_element_type=jnp.float32).astype(jnp.bfloat16)
    key_new = key_new.reshape(BATCH, KVHEADS, HEAD)
    value_new = jnp.dot(tokens, w_value, preferred_element_type=jnp.float32).astype(jnp.bfloat16)
    value_new = value_new.reshape(BATCH, KVHEADS, HEAD)

    def one_sequence(item):
        q_seq, key_seq, value_seq, key_last, value_last, seq_len = item
        q_wide = q_seq.astype(jnp.float32)
        scores = jnp.einsum("grd,gtd->grt", q_wide, key_seq.astype(jnp.float32)) * SCALE
        score_new = jnp.einsum("grd,gd->gr", q_wide, key_last.astype(jnp.float32)) * SCALE
        positions = jnp.arange(CONTEXT)
        scores = jnp.where(positions < seq_len, scores, -jnp.inf)
        score_max = jnp.maximum(jnp.max(scores, axis=-1), score_new)
        weights = jnp.exp(scores - score_max[..., None])
        weight_new = jnp.exp(score_new - score_max)
        denom_sum = jnp.sum(weights, axis=-1) + weight_new
        weighted_sum = jnp.einsum("grt,gtd->grd", weights.astype(jnp.bfloat16).astype(jnp.float32), value_seq.astype(jnp.float32))
        weighted_sum = weighted_sum + weight_new.astype(jnp.bfloat16).astype(jnp.float32)[..., None] * value_last.astype(jnp.float32)[:, None, :]
        return (weighted_sum / denom_sum[..., None]).astype(jnp.bfloat16)

    attended = lax.map(one_sequence, (queries, key_cache, value_cache, key_new, value_new, lengths))
    mixed_sum = jnp.dot(attended.reshape(BATCH, QHEADS * HEAD), w_out, preferred_element_type=jnp.float32)
    out_tokens = (tokens.astype(jnp.float32) + mixed_sum).astype(jnp.bfloat16)
    return (out_tokens, key_new, value_new)
```

```python
import functools

import jax
import jax.numpy as jnp
from jax import lax
from jax.experimental import pallas as pl
from jax.experimental.pallas import tpu as pltpu
from jax.sharding import PartitionSpec as P

MESH = pl.DeviceIdType.MESH
F32 = jnp.float32
BF16 = jnp.bfloat16
MIB = 1 << 20


def coordinates():
    y = lax.axis_index("heads")
    model = lax.axis_index("model")
    return y, model, model // 2, model % 2


def enter(others):
    y, model, _, _ = coordinates()
    me = y * 4 + model
    barrier = pltpu.get_barrier_semaphore()
    for offset in others:
        peer = (me + offset) % 8
        pl.semaphore_signal(barrier, inc=1, device_id={"heads": peer // 4, "model": peer % 4}, device_id_type=MESH)
    pl.semaphore_wait(barrier, len(others))


def query_kernel(groups, cols, depth, slots, kv_depth, kv_slots, x_ref, wq_ref, wk_ref, wv_ref, q_ref, kn_ref, vn_ref, wbuf, kvbuf, acc, kvacc, qs, kvs, kv_all,
                 w_sem, kv_sem, q_send, q_recv, kv_send, kv_recv, self_sem):
    y, model, _, _ = coordinates()
    me = y * 4 + model
    width = x_ref.shape[1]
    steps = width // depth
    kv_steps = width // kv_depth
    total = groups * steps

    def w_copy(i):
        g, k = i // steps, i % steps
        return pltpu.make_async_copy(wq_ref.at[pl.ds(k * depth, depth), pl.ds(g * cols, cols)], wbuf.at[i % slots], w_sem.at[i % slots])

    def kv_copy(ref, col, k):
        return pltpu.make_async_copy(ref.at[pl.ds(k * kv_depth, kv_depth), pl.ds(col * 128, 128)], kvbuf.at[k % kv_slots], kv_sem.at[k % kv_slots])

    def kv_start(k):
        @pl.when(model < 2)
        def _():
            kv_copy(wk_ref, model % 2, k).start()

        @pl.when(model >= 2)
        def _():
            kv_copy(wv_ref, model % 2, k).start()

    for k in range(kv_slots):
        kv_start(k)
    for i in range(slots):
        w_copy(i).start()

    enter(range(1, 8))

    kvacc[...] = jnp.zeros_like(kvacc)

    @pl.loop(0, kv_steps)
    def _(k):
        kv_copy(wk_ref, 0, k).wait()
        kvacc[...] += jnp.dot(x_ref[:, pl.ds(pl.multiple_of(k * kv_depth, 128), kv_depth)], kvbuf[k % kv_slots], preferred_element_type=F32)

        @pl.when(k + kv_slots < kv_steps)
        def _():
            kv_start(k + kv_slots)

    kvs[...] = kvacc[...].astype(BF16)

    def kv_send_copy(offset):
        peer = (model + offset) % 4
        return pltpu.make_async_remote_copy(
            src_ref=kvs.at[pl.ds(peer * 32, 32)], dst_ref=kv_all.at[model], send_sem=kv_send.at[offset], recv_sem=kv_recv.at[model],
            device_id={"heads": y, "model": peer}, device_id_type=MESH)

    for offset in range(1, 4):
        kv_send_copy(offset).start()
    kv_self = pltpu.make_async_copy(kvs.at[pl.ds(model * 32, 32)], kv_all.at[model], self_sem.at[0])
    kv_self.start()

    per_group = cols // 256

    def q_copy(g, h, offset):
        head = g * per_group + h
        peer = (me + offset) % 8
        rows = (peer % 4) * 2 + peer // 4
        return pltpu.make_async_remote_copy(
            src_ref=qs.at[head, pl.ds(rows * 16, 16)], dst_ref=q_ref.at[me * 6 + head],
            send_sem=q_send.at[head * 8 + offset], recv_sem=q_recv.at[me * 6 + head],
            device_id={"heads": peer // 4, "model": peer % 4}, device_id_type=MESH)

    def q_self(head):
        return pltpu.make_async_copy(qs.at[head, pl.ds((model * 2 + y) * 16, 16)], q_ref.at[me * 6 + head], self_sem.at[1 + head])

    @pl.loop(0, total)
    def _(i):
        g, k = i // steps, i % steps
        w_copy(i).wait()
        part = jnp.dot(x_ref[:, pl.ds(pl.multiple_of(k * depth, 128), depth)], wbuf[i % slots], preferred_element_type=F32)

        @pl.when(k == 0)
        def _():
            acc[...] = part

        @pl.when(k > 0)
        def _():
            acc[...] += part

        @pl.when(i + slots < total)
        def _():
            w_copy(i + slots).start()

        @pl.when(k == steps - 1)
        def _():
            for h in range(per_group):
                qs[g * per_group + h] = acc[:, h * 256:(h + 1) * 256].astype(BF16)
            for h in range(per_group):
                for offset in range(1, 8):
                    q_copy(g, h, offset).start()
                q_self(g * per_group + h).start()

    kv_self.wait()
    for offset in range(1, 4):
        kv_send_copy(offset).wait_send()
        src = (model + offset) % 4
        pltpu.make_async_copy(kv_all.at[src], kv_all.at[src], kv_recv.at[src]).wait()
    kn_ref[:, :128] = kv_all[0]
    kn_ref[:, 128:] = kv_all[1]
    vn_ref[:, :128] = kv_all[2]
    vn_ref[:, 128:] = kv_all[3]

    @pl.loop(0, 6)
    def _(head):
        q_self(head).wait()
        for offset in range(1, 8):
            q_copy(0, head, offset).wait_send()
            src = (me + offset) % 8
            pltpu.make_async_copy(q_ref.at[src * 6 + head], q_ref.at[src * 6 + head], q_recv.at[src * 6 + head]).wait()


def project_queries(tokens, w_query, w_key, w_value):
    rows, width = tokens.shape
    groups, cols, depth, slots = 3, 512, 2304, 6
    kv_depth, kv_slots = 4608, 2
    vmem = pl.BlockSpec(memory_space=pltpu.VMEM)
    hbm = pl.BlockSpec(memory_space=pl.ANY)
    return pl.pallas_call(
        functools.partial(query_kernel, groups, cols, depth, slots, kv_depth, kv_slots),
        out_shape=(jax.ShapeDtypeStruct((48, 16, 256), BF16), jax.ShapeDtypeStruct((32, 256), BF16), jax.ShapeDtypeStruct((32, 256), BF16)),
        in_specs=[vmem, hbm, hbm, hbm],
        out_specs=(vmem, vmem, vmem),
        scratch_shapes=[
            pltpu.VMEM((slots, depth, cols), BF16),
            pltpu.VMEM((kv_slots, kv_depth, 128), BF16),
            pltpu.VMEM((rows, cols), F32),
            pltpu.VMEM((rows, 128), F32),
            pltpu.VMEM((6, rows, 256), BF16),
            pltpu.VMEM((rows, 128), BF16),
            pltpu.VMEM((4, 32, 128), BF16),
            pltpu.SemaphoreType.DMA((slots,)),
            pltpu.SemaphoreType.DMA((kv_slots,)),
            pltpu.SemaphoreType.DMA((48,)),
            pltpu.SemaphoreType.DMA((48,)),
            pltpu.SemaphoreType.DMA((4,)),
            pltpu.SemaphoreType.DMA((4,)),
            pltpu.SemaphoreType.DMA((7,)),
        ],
        compiler_params=pltpu.CompilerParams(collective_id=0, has_side_effects=True, vmem_limit_bytes=48 * MIB),
        cost_estimate=pl.CostEstimate(flops=2 * rows * width * 1664, bytes_accessed=width * 1664 * 2, transcendentals=0),
        name="query",
    )(tokens, w_query, w_key, w_value)


ITEM = 1024


def attend_kernel(slots, len_ref, q_ref, kn_ref, vn_ref, key_ref, value_ref, o_ref, kbuf, vbuf, qf, of, knf, vnf, sbuf, acc, m_ref, l_ref, items, k_sem, v_sem):
    y = lax.axis_index("heads")
    first_seq = y * 16
    scale = 256 ** -0.5

    def list_seq(s, count):
        length = len_ref[first_seq + s]
        chunks = (length + ITEM - 1) // ITEM
        for c in range(4):
            @pl.when(c < chunks)
            def _():
                items[count + c] = s * 4 + c
        return count + chunks

    total = lax.fori_loop(0, 16, list_seq, jnp.int32(0))

    def where_is(i):
        entry = items[i]
        s, c = entry // 4, entry % 4
        left = jnp.minimum(len_ref[first_seq + s] - c * ITEM, ITEM)
        return s, c, pl.multiple_of((left + 15) // 16 * 16, 16)

    def copy(i, ref, buf, sem):
        s, c, size = where_is(i)
        slot = i % slots
        return pltpu.make_async_copy(ref.at[first_seq + s, 0, pl.ds(pl.multiple_of(c * ITEM, ITEM), size)], buf.at[slot, pl.ds(0, size)], sem.at[slot])

    def k_copy(i):
        return copy(i, key_ref, kbuf, k_sem)

    def v_copy(i):
        return copy(i, value_ref, vbuf, v_sem)

    for i in range(slots - 1):
        @pl.when(i < total)
        def _():
            k_copy(i).start()
    for i in range(slots):
        vbuf[i] = jnp.zeros((ITEM, 256), BF16)
        if i < slots - 1:
            @pl.when(i < total)
            def _():
                v_copy(i).start()

    for part in range(2):
        qf[part] = q_ref[:, :, part * 128:(part + 1) * 128].reshape(768, 128).astype(F32)
    knf[...] = kn_ref[...].astype(F32)
    vnf[...] = vn_ref[...].astype(F32)
    m_ref[...] = jnp.zeros_like(m_ref)
    l_ref[...] = jnp.ones_like(l_ref)
    acc[...] = jnp.zeros_like(acc)

    def query(s):
        return jnp.concatenate([qf[part, pl.ds(s, 48, stride=16), :] for part in range(2)], axis=1)

    def scores(i):
        s, _, _ = where_is(i)
        q = query(s).astype(BF16)
        sbuf[i % 2] = lax.dot_general(q, kbuf[i % slots], (((1,), (1,)), ((), ())), preferred_element_type=F32)

    k_copy(0).wait()
    scores(0)

    @pl.loop(0, total)
    def _(i):
        @pl.when(i + slots - 1 < total)
        def _():
            k_copy(i + slots - 1).start()
            v_copy(i + slots - 1).start()

        after = jnp.minimum(i + 1, total - 1)

        @pl.when(i + 1 < total)
        def _():
            k_copy(i + 1).wait()
        v_copy(i).wait()

        s_after, _, _ = where_is(after)
        q_after = query(s_after).astype(BF16)
        s_next = lax.dot_general(q_after, kbuf[after % slots], (((1,), (1,)), ((), ())), preferred_element_type=F32)

        s, c, _ = where_is(i)
        left = len_ref[first_seq + s] - c * ITEM
        fresh = c == 0
        q_now = query(s)
        kn = knf[pl.ds(first_seq + s, 1), :]
        vn = vnf[pl.ds(first_seq + s, 1), :]
        score_new = jnp.sum(q_now * kn, axis=1, keepdims=True) * scale
        m_old = jnp.where(fresh, score_new, m_ref[:, :1])
        l_old = jnp.where(fresh, 1.0, l_ref[:, :1])
        acc_old = jnp.where(fresh, jnp.broadcast_to(vn, acc.shape), acc[...])
        x = sbuf[i % 2] * scale
        x = jnp.where(lax.broadcasted_iota(jnp.int32, x.shape, 1) < left, x, -jnp.inf)
        m_now = jnp.maximum(m_old, jnp.max(x, axis=1, keepdims=True))
        alpha = jnp.exp(m_old - m_now)
        p = jnp.exp(x - m_now)
        l_now = l_old * alpha + jnp.sum(p, axis=1, keepdims=True)
        acc_now = acc_old * alpha + jnp.dot(p.astype(BF16), vbuf[i % slots], preferred_element_type=F32)
        m_ref[...] = jnp.broadcast_to(m_now, m_ref.shape)
        l_ref[...] = jnp.broadcast_to(l_now, l_ref.shape)
        acc[...] = acc_now
        result = acc_now / l_now
        for part in range(2):
            of[part, pl.ds(pl.multiple_of(s * 48, 8), 48), :] = result[:, part * 128:(part + 1) * 128]
        sbuf[(i + 1) % 2] = s_next

    for h in range(48):
        for part in range(2):
            start = (h % 6) * 256 + part * 128
            o_ref[h // 6, :, start:start + 128] = of[part, pl.ds(h, 16, stride=48), :].astype(BF16)


def attend(lengths, queries, key_new, value_new, key_cache, value_cache):
    slots = 10
    vmem = pl.BlockSpec(memory_space=pltpu.VMEM)
    hbm = pl.BlockSpec(memory_space=pl.ANY)
    return pl.pallas_call(
        functools.partial(attend_kernel, slots),
        out_shape=jax.ShapeDtypeStruct((8, 16, 1536), BF16),
        in_specs=[pl.BlockSpec(memory_space=pltpu.SMEM), vmem, vmem, vmem, hbm, hbm],
        out_specs=vmem,
        scratch_shapes=[
            pltpu.VMEM((slots, ITEM, 256), BF16),
            pltpu.VMEM((slots, ITEM, 256), BF16),
            pltpu.VMEM((2, 768, 128), F32),
            pltpu.VMEM((2, 768, 128), F32),
            pltpu.VMEM((32, 256), F32),
            pltpu.VMEM((32, 256), F32),
            pltpu.VMEM((2, 48, ITEM), F32),
            pltpu.VMEM((48, 256), F32),
            pltpu.VMEM((48, 128), F32),
            pltpu.VMEM((48, 128), F32),
            pltpu.SMEM((64,), jnp.int32),
            pltpu.SemaphoreType.DMA((slots,)),
            pltpu.SemaphoreType.DMA((slots,)),
        ],
        compiler_params=pltpu.CompilerParams(vmem_limit_bytes=40 * MIB),
        cost_estimate=pl.CostEstimate(flops=4 * 16 * 48 * 2048 * 256, bytes_accessed=16 * 2048 * 1024, transcendentals=16 * 48 * 2048),
        name="attend",
    )(lengths, queries, key_new, value_new, key_cache, value_cache)


LAGS = (1, 4, 7, 10, 13)


def mix_kernel(chunk, slots, o_ref, w_ref, x_ref, out_ref, o_all, wbuf, xrows, part, r0, r1, r2,
               w_sem, x_sem, o_send, o_recv, s0s, s0r, s1s, s1r, s2s, s2r, g1s, g1r, g2s, g2r, g3s, g3r):
    y, model, x, core = coordinates()
    me = y * 4 + model
    width = w_ref.shape[1]
    chunks = width // chunk
    first, second = x * (1 - core) + y * core, y * (1 - core) + x * core
    own = core * 4 + first * 2 + second
    flip_x = {"heads": y, "model": (1 - x) * 2 + core}
    partner = {"heads": y, "model": x * 2 + 1 - core}
    along_first = {"heads": y * (1 - core) + (1 - y) * core, "model": ((1 - x) * (1 - core) + x * core) * 2 + core}
    along_second = {"heads": (1 - y) * (1 - core) + y * core, "model": (x * (1 - core) + (1 - x) * core) * 2 + core}

    def w_copy(t):
        return pltpu.make_async_copy(w_ref.at[:, pl.ds(pl.multiple_of(t * chunk, chunk), chunk)], wbuf.at[t % slots], w_sem.at[t % slots])

    for t in range(slots):
        w_copy(t).start()
    x_copy = pltpu.make_async_copy(x_ref.at[pl.ds(own * 16, 16)], xrows, x_sem)
    x_copy.start()

    enter(range(1, 8))

    mine = model * 2 + y

    def o_copy(offset):
        peer = (me + offset) % 8
        return pltpu.make_async_remote_copy(
            src_ref=o_ref.at[peer], dst_ref=o_all.at[pl.ds(mine * 16, 16)], send_sem=o_send.at[offset], recv_sem=o_recv.at[me],
            device_id={"heads": peer // 4, "model": peer % 4}, device_id_type=MESH)

    for offset in range(1, 8):
        o_copy(offset).start()
    o_self = pltpu.make_async_copy(o_ref.at[me], o_all.at[pl.ds(mine * 16, 16)], o_send.at[0])
    o_self.start()
    o_self.wait()
    for offset in range(1, 8):
        src = (me + offset) % 8
        block = o_all.at[pl.ds(((src % 4) * 2 + src // 4) * 16, 16)]
        pltpu.make_async_copy(block, block, o_recv.at[src]).wait()
    x_copy.wait()

    def remote(src, dst, send, recv, device):
        return pltpu.make_async_remote_copy(src_ref=src, dst_ref=dst, send_sem=send, recv_sem=recv, device_id=device, device_id_type=MESH)

    half, quarter = core * 64, core * 64 + first * 32
    eighth = quarter + second * 16
    cols = lambda j: pl.ds(pl.multiple_of(j * chunk, chunk), chunk)

    def s0(j):
        return remote(part.at[j, pl.ds((1 - core) * 64, 64)], r0.at[j], s0s.at[j], s0r.at[j], partner)

    def s1(j):
        return remote(part.at[j, pl.ds(half + (1 - first) * 32, 32)], r1.at[j], s1s.at[j], s1r.at[j], along_first)

    def s2(j):
        return remote(part.at[j, pl.ds(quarter + (1 - second) * 16, 16)], r2.at[j], s2s.at[j], s2r.at[j], along_second)

    def g1(j):
        piece = out_ref.at[pl.ds(eighth, 16), cols(j)]
        return remote(piece, piece, g1s.at[j], g1r.at[j], along_second)

    def g2(j):
        piece = out_ref.at[pl.ds(quarter, 32), cols(j)]
        return remote(piece, piece, g2s.at[j], g2r.at[j], along_first)

    def g3(j):
        piece = out_ref.at[pl.ds(half, 64), cols(j)]
        return remote(piece, piece, g3s.at[j], g3r.at[j], partner)

    def arrived(ref, sem):
        pltpu.make_async_copy(ref, ref, sem).wait()

    def at(t, lag, body):
        j = t - lag

        @pl.when(jnp.logical_and(j >= 0, j < chunks))
        def _():
            body(j)

    def stage5(j):
        arrived(out_ref.at[pl.ds(core * 64 + (1 - first) * 32, 32), cols(j)], g2r.at[j])
        g3(j).start()

    def stage4(j):
        arrived(out_ref.at[pl.ds(quarter + (1 - second) * 16, 16), cols(j)], g1r.at[j])
        g2(j).start()

    def stage3(j):
        arrived(r2.at[j], s2r.at[j])
        total = part[j, pl.ds(pl.multiple_of(eighth, 16), 16)] + r2[j]
        out_ref[pl.ds(pl.multiple_of(eighth, 16), 16), cols(j)] = (xrows[:, cols(j)].astype(F32) + total).astype(BF16)
        g1(j).start()

    def stage2(j):
        arrived(r1.at[j], s1r.at[j])
        part[j, pl.ds(pl.multiple_of(quarter, 16), 32)] += r1[j]
        s2(j).start()

    def stage1(j):
        arrived(r0.at[j], s0r.at[j])
        part[j, pl.ds(pl.multiple_of(half, 16), 64)] += r0[j]
        s1(j).start()

    def stage0(j):
        w_copy(j).wait()
        part[j] = jnp.dot(o_all[...], wbuf[j % slots], preferred_element_type=F32)

        @pl.when(j + slots < chunks)
        def _():
            w_copy(j + slots).start()
        s0(j).start()

    @pl.loop(0, chunks + LAGS[-1])
    def _(t):
        at(t, 0, stage0)
        at(t, LAGS[0], stage1)
        at(t, LAGS[1], stage2)
        at(t, LAGS[2], stage3)
        at(t, LAGS[3], stage4)
        at(t, LAGS[4], stage5)

    for offset in range(1, 8):
        o_copy(offset).wait_send()

    @pl.loop(0, chunks)
    def _(j):
        arrived(out_ref.at[pl.ds((1 - core) * 64, 64), cols(j)], g3r.at[j])
        for copy in (s0, s1, s2, g1, g2, g3):
            copy(j).wait_send()


def mix(attended, w_out, tokens):
    depth, width = w_out.shape
    chunk, slots = 512, 8
    chunks = width // chunk
    vmem = pl.BlockSpec(memory_space=pltpu.VMEM)
    hbm = pl.BlockSpec(memory_space=pl.ANY)
    sems = pltpu.SemaphoreType.DMA((chunks,))
    return pl.pallas_call(
        functools.partial(mix_kernel, chunk, slots),
        out_shape=jax.ShapeDtypeStruct((128, width), BF16),
        in_specs=[vmem, hbm, hbm],
        out_specs=vmem,
        scratch_shapes=[
            pltpu.VMEM((128, depth), BF16),
            pltpu.VMEM((slots, depth, chunk), BF16),
            pltpu.VMEM((16, width), BF16),
            pltpu.VMEM((chunks, 128, chunk), F32),
            pltpu.VMEM((chunks, 64, chunk), F32),
            pltpu.VMEM((chunks, 32, chunk), F32),
            pltpu.VMEM((chunks, 16, chunk), F32),
            pltpu.SemaphoreType.DMA((slots,)),
            pltpu.SemaphoreType.DMA,
            pltpu.SemaphoreType.DMA((8,)),
            pltpu.SemaphoreType.DMA((8,)),
        ] + [sems] * 12,
        compiler_params=pltpu.CompilerParams(collective_id=1, has_side_effects=True, vmem_limit_bytes=56 * MIB),
        cost_estimate=pl.CostEstimate(flops=2 * 128 * depth * width, bytes_accessed=depth * width * 2, transcendentals=0),
        name="mix",
    )(attended, w_out, tokens)


def solution(mesh):
    def local_step(tokens, w_query, w_key, w_value, w_out, key_cache, value_cache, lengths):
        queries, key_new, value_new = project_queries(tokens, w_query, w_key, w_value)
        attended = attend(lengths, queries, key_new, value_new, key_cache, value_cache)
        out_tokens = mix(attended, w_out, tokens)
        return (out_tokens, key_new.reshape(32, 1, 256), value_new.reshape(32, 1, 256))

    cache_spec = P(("replica", "model"), None, None, None)
    new_spec = P(("replica", "model"), None, None)
    return jax.shard_map(
        local_step,
        mesh=mesh,
        in_specs=(P("replica", None), P(None, ("heads", "model")), P(None, None), P(None, None), P(("heads", "model"), None), cache_spec, cache_spec, P(("replica", "model"))),
        out_specs=(P("replica", None), new_spec, new_spec),
        check_vma=False,
    )
```

```python
import functools

import jax
import jax.numpy as jnp
from jax import lax
from jax.experimental import pallas as pl
from jax.experimental.pallas import tpu as pltpu
from jax.sharding import PartitionSpec as P

MESH = pl.DeviceIdType.MESH
F32 = jnp.float32
BF16 = jnp.bfloat16
MIB = 1 << 20


def coordinates():
    y = lax.axis_index("heads")
    model = lax.axis_index("model")
    return y, model, model // 2, model % 2


def enter(others):
    y, model, _, _ = coordinates()
    me = y * 4 + model
    barrier = pltpu.get_barrier_semaphore()
    for offset in others:
        peer = (me + offset) % 8
        pl.semaphore_signal(barrier, inc=1, device_id={"heads": peer // 4, "model": peer % 4}, device_id_type=MESH)
    pl.semaphore_wait(barrier, len(others))


def query_kernel(groups, cols, depth, slots, kv_depth, x_ref, wq_ref, wk_ref, wv_ref, q_ref, kn_ref, vn_ref, xbuf, wbuf, kvbuf, acc, kvacc, qs, kvs, kv_all,
                 x_sem, w_sem, kv_sem, q_send, q_recv, kv_send, kv_recv, self_sem):
    y, model, _, _ = coordinates()
    me = y * 4 + model
    width = x_ref.shape[1]
    steps = width // depth
    kv_steps = width // kv_depth
    total = groups * steps

    def w_copy(i):
        g, k = i // steps, i % steps
        return pltpu.make_async_copy(wq_ref.at[pl.ds(k * depth, depth), pl.ds(g * cols, cols)], wbuf.at[i % slots], w_sem.at[i % slots])

    def x_copy(k):
        part = pl.ds(pl.multiple_of(k * depth, 128), depth)
        return pltpu.make_async_copy(x_ref.at[:, part], xbuf.at[:, part], x_sem.at[k])

    def kv_copy(ref, col, k):
        return pltpu.make_async_copy(ref.at[pl.ds(k * kv_depth, kv_depth), pl.ds(col * 128, 128)], kvbuf.at[k], kv_sem.at[k])

    for i in range(max(steps, slots)):
        if i < steps:
            x_copy(i).start()
        if i < slots:
            w_copy(i).start()

    enter(range(1, 8))

    per_group = cols // 256

    def q_copy(g, h, offset):
        head = g * per_group + h
        peer = (me + offset) % 8
        rows = (peer % 4) * 2 + peer // 4
        return pltpu.make_async_remote_copy(
            src_ref=qs.at[head, pl.ds(rows * 16, 16)], dst_ref=q_ref.at[me * 6 + head],
            send_sem=q_send.at[head * 8 + offset], recv_sem=q_recv.at[me * 6 + head],
            device_id={"heads": peer // 4, "model": peer % 4}, device_id_type=MESH)

    def q_self(head):
        return pltpu.make_async_copy(qs.at[head, pl.ds((model * 2 + y) * 16, 16)], q_ref.at[me * 6 + head], self_sem.at[1 + head])

    @pl.loop(0, total)
    def _(i):
        g, k = i // steps, i % steps

        @pl.when(i < steps)
        def _():
            x_copy(i).wait()

        w_copy(i).wait()
        part = jnp.dot(xbuf[:, pl.ds(pl.multiple_of(k * depth, 128), depth)], wbuf[i % slots], preferred_element_type=F32)

        @pl.when(k == 0)
        def _():
            acc[...] = part

        @pl.when(k > 0)
        def _():
            acc[...] += part

        @pl.when(i + slots < total)
        def _():
            w_copy(i + slots).start()

        for n in range(kv_steps):
            @pl.when(i == total - kv_steps + n - 1)
            def _():
                @pl.when(model < 2)
                def _():
                    kv_copy(wk_ref, model % 2, n).start()

                @pl.when(model >= 2)
                def _():
                    kv_copy(wv_ref, model % 2, n).start()

        @pl.when(k == steps - 1)
        def _():
            for h in range(per_group):
                qs[g * per_group + h] = acc[:, h * 256:(h + 1) * 256].astype(BF16)
            for h in range(per_group):
                for offset in (7, 6, 5, 4, 3, 2, 1):
                    q_copy(g, h, offset).start()
                q_self(g * per_group + h).start()

    kvacc[...] = jnp.zeros_like(kvacc)

    @pl.loop(0, kv_steps)
    def _(k):
        kv_copy(wk_ref, 0, k).wait()
        kvacc[...] += jnp.dot(xbuf[:, pl.ds(pl.multiple_of(k * kv_depth, 128), kv_depth)], kvbuf[k], preferred_element_type=F32)

    kvs[...] = kvacc[...].astype(BF16)

    def kv_send_copy(offset):
        peer = (model + offset) % 4
        return pltpu.make_async_remote_copy(
            src_ref=kvs.at[pl.ds(peer * 32, 32)], dst_ref=kv_all.at[model], send_sem=kv_send.at[offset], recv_sem=kv_recv.at[model],
            device_id={"heads": y, "model": peer}, device_id_type=MESH)

    for offset in (2, 3, 1):
        kv_send_copy(offset).start()
    kv_self = pltpu.make_async_copy(kvs.at[pl.ds(model * 32, 32)], kv_all.at[model], self_sem.at[0])
    kv_self.start()

    @pl.loop(0, 6)
    def _(head):
        q_self(head).wait()
        for offset in range(1, 8):
            q_copy(0, head, offset).wait_send()
            src = (me + offset) % 8
            pltpu.make_async_copy(q_ref.at[src * 6 + head], q_ref.at[src * 6 + head], q_recv.at[src * 6 + head]).wait()

    kv_self.wait()
    for offset in range(1, 4):
        kv_send_copy(offset).wait_send()
        src = (model + offset) % 4
        pltpu.make_async_copy(kv_all.at[src], kv_all.at[src], kv_recv.at[src]).wait()
    kn_ref[:, :128] = kv_all[0]
    kn_ref[:, 128:] = kv_all[1]
    vn_ref[:, :128] = kv_all[2]
    vn_ref[:, 128:] = kv_all[3]


def project_queries(tokens, w_query, w_key, w_value):
    rows, width = tokens.shape
    groups, cols, depth, slots = 6, 256, 4608, 6
    kv_depth = 4608
    vmem = pl.BlockSpec(memory_space=pltpu.VMEM)
    hbm = pl.BlockSpec(memory_space=pltpu.HBM)
    return pl.pallas_call(
        functools.partial(query_kernel, groups, cols, depth, slots, kv_depth),
        out_shape=(jax.ShapeDtypeStruct((48, 16, 256), BF16), jax.ShapeDtypeStruct((32, 256), BF16), jax.ShapeDtypeStruct((32, 256), BF16)),
        in_specs=[hbm, hbm, hbm, hbm],
        out_specs=(vmem, vmem, vmem),
        scratch_shapes=[
            pltpu.VMEM((rows, width), BF16),
            pltpu.VMEM((slots, depth, cols), BF16),
            pltpu.VMEM((width // kv_depth, kv_depth, 128), BF16),
            pltpu.VMEM((rows, cols), F32),
            pltpu.VMEM((rows, 128), F32),
            pltpu.VMEM((6, rows, 256), BF16),
            pltpu.VMEM((rows, 128), BF16),
            pltpu.VMEM((4, 32, 128), BF16),
            pltpu.SemaphoreType.DMA((width // depth,)),
            pltpu.SemaphoreType.DMA((slots,)),
            pltpu.SemaphoreType.DMA((width // kv_depth,)),
            pltpu.SemaphoreType.DMA((48,)),
            pltpu.SemaphoreType.DMA((48,)),
            pltpu.SemaphoreType.DMA((4,)),
            pltpu.SemaphoreType.DMA((4,)),
            pltpu.SemaphoreType.DMA((7,)),
        ],
        compiler_params=pltpu.CompilerParams(collective_id=0, has_side_effects=True, vmem_limit_bytes=48 * MIB),
        cost_estimate=pl.CostEstimate(flops=2 * rows * width * 1664, bytes_accessed=width * 1664 * 2, transcendentals=0),
        name="query",
    )(*(pltpu.with_memory_space_constraint(a, pltpu.HBM) for a in (tokens, w_query, w_key, w_value)))


ITEM = 1024


def attend_kernel(slots, len_ref, q_ref, kn_ref, vn_ref, key_ref, value_ref, o_ref, kn_out, vn_out, kbuf, vbuf, perm, back, qs, os, sn, vnf, sbuf, pbuf, acc, m_ref, l_ref, a_ref, r_ref, items, left, k_sem, v_sem):
    y = lax.axis_index("heads")
    first_seq = y * 16
    power = 256 ** -0.5 * 1.4426950408889634

    def list_seq(s, count):
        length = len_ref[first_seq + s]
        chunks = (length + ITEM - 1) // ITEM
        for c in range(4):
            @pl.when(c < chunks)
            def _():
                items[count + c] = s * 4 + c
                left[count + c] = length - c * ITEM
        return count + chunks

    total = lax.fori_loop(0, 16, list_seq, jnp.int32(0))
    items[total] = items[total - 1] // 4 * 4 + 3
    left[total] = 0
    pairs = (total + 1) // 2

    def copy(i, ref, buf, sem):
        entry = items[i]
        slot = i % slots
        size = pl.multiple_of((jnp.minimum(left[i], ITEM) + 15) // 16 * 16, 16)
        return pltpu.make_async_copy(ref.at[first_seq + entry // 4, 0, pl.ds(pl.multiple_of(entry % 4 * ITEM, ITEM), size)], buf.at[slot, pl.ds(0, size)], sem.at[slot])

    def k_copy(i):
        return copy(i, key_ref, kbuf, k_sem)

    def v_copy(i):
        return copy(i, value_ref, vbuf, v_sem)

    for i in range(slots - 2):
        @pl.when(i < total)
        def _():
            k_copy(i).start()
    for i in range(slots):
        vbuf[i] = jnp.zeros((ITEM, 256), BF16)
        if i < slots - 2:
            @pl.when(i < total)
            def _():
                v_copy(i).start()

    kn_out[...] = kn_ref[...]
    vn_out[...] = vn_ref[...]
    column = lax.broadcasted_iota(jnp.int32, (48, 768), 1)
    row = lax.broadcasted_iota(jnp.int32, (48, 768), 0)
    for n in range(16):
        perm[n * 48:(n + 1) * 48] = jnp.where(column == row * 16 + n, 1.0, 0.0).astype(BF16)
        back[n * 48:(n + 1) * 48] = jnp.where(column == row % 16 * 48 + row // 16 + 3 * n, 1.0, 0.0).astype(BF16)
    qs[...] = jnp.dot(perm[...], q_ref[...].reshape(768, 256), preferred_element_type=F32).astype(BF16)
    vnf[...] = vn_ref[pl.ds(pl.multiple_of(first_seq, 16), 16), :].astype(F32)
    knf = kn_ref[pl.ds(pl.multiple_of(first_seq, 16), 16), :].astype(F32)
    for n in range(16):
        rows = slice(n * 48, (n + 1) * 48)
        sn[rows] = jnp.broadcast_to(jnp.sum(qs[rows].astype(F32) * knf[n:n + 1], axis=1, keepdims=True), (48, 128))
    m_ref[...] = jnp.zeros_like(m_ref)
    l_ref[...] = jnp.ones_like(l_ref)
    acc[...] = jnp.zeros_like(acc)

    def rows_of(entry):
        return pl.ds(pl.multiple_of(entry // 4 * 48, 16), 48)

    def score(i):
        return lax.dot_general(qs[rows_of(items[i]), :], kbuf[i % slots], (((1,), (1,)), ((), ())), preferred_element_type=F32)

    lane = lax.broadcasted_iota(jnp.int32, (48, 128), 1)

    halves = (slice(0, 128), slice(128, 256))
    chunks = [slice(n * 128, (n + 1) * 128) for n in range(ITEM // 128)]

    def pair_scores(pair, turn):
        for n in range(2):
            sbuf[turn, n] = score(2 * pair + n)

    def weigh(pair, turn):
        m, l = m_ref[...], l_ref[...]
        for n in range(2):
            i = 2 * pair + n
            entry = items[i]
            fresh = entry % 4 == 0
            m_old = jnp.where(fresh, sn[rows_of(entry), :], m)
            x = [jnp.where(lane < left[i] - c.start, sbuf[turn, n, :, c], -jnp.inf) for c in chunks]
            top = functools.reduce(jnp.maximum, x)
            m = jnp.maximum(m_old, jnp.broadcast_to(jnp.max(top, axis=1, keepdims=True), (48, 128)))
            alpha = jnp.exp2((m_old - m) * power)
            p = [jnp.exp2((v - m) * power) for v in x]
            l = jnp.where(fresh, 1.0, l) * alpha + jnp.broadcast_to(jnp.sum(functools.reduce(jnp.add, p), axis=1, keepdims=True), (48, 128))
            a_ref[turn, n] = alpha
            r_ref[turn, n] = l
            for c, v in zip(chunks, p):
                pbuf[turn, n, :, c] = v.astype(BF16)
        m_ref[...] = m
        l_ref[...] = l

    def blend(pair, turn):
        for n in range(2):
            i = 2 * pair + n
            entry = items[i]
            added = jnp.dot(pbuf[turn, n], vbuf[i % slots], preferred_element_type=F32)
            alpha = a_ref[turn, n]
            inverse = 1.0 / r_ref[turn, n]
            fresh_row = vnf[pl.ds(entry // 4, 1), :]
            for h in halves:
                now = jnp.where(entry % 4 == 0, jnp.broadcast_to(fresh_row[:, h], (48, 128)), acc[:, h]) * alpha + added[:, h]
                acc[:, h] = now
                os[rows_of(entry), h] = (now * inverse).astype(BF16)

    def arrive(copy, pair):
        for n in range(2):
            @pl.when(2 * pair + n < total)
            def _():
                copy(2 * pair + n).wait()

    arrive(k_copy, 0)
    pair_scores(0, 0)
    weigh(0, 0)
    arrive(k_copy, 1)
    pair_scores(jnp.minimum(1, pairs - 1), 1)

    @pl.loop(0, pairs)
    def _(pair):
        for n in range(2):
            i = 2 * pair + slots - 2 + n

            @pl.when(i < total)
            def _():
                k_copy(i).start()
                v_copy(i).start()

        arrive(k_copy, pair + 2)
        arrive(v_copy, pair)
        turn = pair % 2
        blend(pair, turn)
        weigh(jnp.minimum(pair + 1, pairs - 1), 1 - turn)
        pair_scores(jnp.minimum(pair + 2, pairs - 1), turn)

    mixed = jnp.dot(back[...], os[...], preferred_element_type=F32).astype(BF16)
    for h in range(48):
        o_ref[h // 6, :, (h % 6) * 256:(h % 6 + 1) * 256] = mixed[h * 16:(h + 1) * 16]


def attend(lengths, queries, key_new, value_new, key_cache, value_cache):
    slots = 12
    vmem = pl.BlockSpec(memory_space=pltpu.VMEM)
    hbm = pl.BlockSpec(memory_space=pltpu.HBM)
    return pl.pallas_call(
        functools.partial(attend_kernel, slots),
        out_shape=(jax.ShapeDtypeStruct((8, 16, 1536), BF16), jax.ShapeDtypeStruct((32, 256), BF16), jax.ShapeDtypeStruct((32, 256), BF16)),
        in_specs=[pl.BlockSpec(memory_space=pltpu.SMEM), vmem, vmem, vmem, hbm, hbm],
        out_specs=(vmem, vmem, vmem),
        scratch_shapes=[
            pltpu.VMEM((slots, ITEM, 256), BF16),
            pltpu.VMEM((slots, ITEM, 256), BF16),
            pltpu.VMEM((768, 768), BF16),
            pltpu.VMEM((768, 768), BF16),
            pltpu.VMEM((768, 256), BF16),
            pltpu.VMEM((768, 256), BF16),
            pltpu.VMEM((768, 128), F32),
            pltpu.VMEM((16, 256), F32),
            pltpu.VMEM((2, 2, 48, ITEM), F32),
            pltpu.VMEM((2, 2, 48, ITEM), BF16),
            pltpu.VMEM((48, 256), F32),
            pltpu.VMEM((48, 128), F32),
            pltpu.VMEM((48, 128), F32),
            pltpu.VMEM((2, 2, 48, 128), F32),
            pltpu.VMEM((2, 2, 48, 128), F32),
            pltpu.SMEM((72,), jnp.int32),
            pltpu.SMEM((72,), jnp.int32),
            pltpu.SemaphoreType.DMA((slots,)),
            pltpu.SemaphoreType.DMA((slots,)),
        ],
        compiler_params=pltpu.CompilerParams(vmem_limit_bytes=40 * MIB),
        cost_estimate=pl.CostEstimate(flops=4 * 16 * 48 * 2048 * 256, bytes_accessed=16 * 2048 * 1024, transcendentals=16 * 48 * 2048),
        name="attend",
    )(lengths, queries, key_new, value_new, key_cache, value_cache)


LAGS = (4, 9, 15, 22, 28)


def mix_kernel(chunk, slots, o_ref, w_ref, x_ref, out_ref, o_all, wbuf, xrows, part, r0, r1, r2,
               w_sem, x_sem, o_send, o_recv, s0s, s0r, s1s, s1r, s2s, s2r, g1s, g1r, g2s, g2r, g3s, g3r):
    y, model, x, core = coordinates()
    me = y * 4 + model
    width = w_ref.shape[1]
    chunks = width // chunk
    first, second = x * (1 - core) + y * core, y * (1 - core) + x * core
    own = core * 4 + first * 2 + second
    flip_x = {"heads": y, "model": (1 - x) * 2 + core}
    partner = {"heads": y, "model": x * 2 + 1 - core}
    along_first = {"heads": y * (1 - core) + (1 - y) * core, "model": ((1 - x) * (1 - core) + x * core) * 2 + core}
    along_second = {"heads": (1 - y) * (1 - core) + y * core, "model": (x * (1 - core) + (1 - x) * core) * 2 + core}

    def w_copy(t):
        return pltpu.make_async_copy(w_ref.at[:, pl.ds(pl.multiple_of(t * chunk, chunk), chunk)], wbuf.at[t % slots], w_sem.at[t % slots])

    for t in range(slots):
        w_copy(t).start()
    x_copy = pltpu.make_async_copy(x_ref.at[pl.ds(own * 16, 16)], xrows, x_sem)
    x_copy.start()

    enter(range(1, 8))

    mine = model * 2 + y

    def o_copy(offset):
        peer = (me + offset) % 8
        return pltpu.make_async_remote_copy(
            src_ref=o_ref.at[peer], dst_ref=o_all.at[pl.ds(mine * 16, 16)], send_sem=o_send.at[offset], recv_sem=o_recv.at[me],
            device_id={"heads": peer // 4, "model": peer % 4}, device_id_type=MESH)

    for offset in range(1, 8):
        o_copy(offset).start()
    o_self = pltpu.make_async_copy(o_ref.at[me], o_all.at[pl.ds(mine * 16, 16)], o_send.at[0])
    o_self.start()
    o_self.wait()
    for offset in range(1, 8):
        src = (me + offset) % 8
        block = o_all.at[pl.ds(((src % 4) * 2 + src // 4) * 16, 16)]
        pltpu.make_async_copy(block, block, o_recv.at[src]).wait()
    x_copy.wait()

    def remote(src, dst, send, recv, device):
        return pltpu.make_async_remote_copy(src_ref=src, dst_ref=dst, send_sem=send, recv_sem=recv, device_id=device, device_id_type=MESH)

    half, quarter = core * 64, core * 64 + first * 32
    eighth = quarter + second * 16
    cols = lambda j: pl.ds(pl.multiple_of(j * chunk, chunk), chunk)

    def s0(j):
        return remote(part.at[j, pl.ds((1 - core) * 64, 64)], r0.at[j], s0s.at[j], s0r.at[j], partner)

    def s1(j):
        return remote(part.at[j, pl.ds(half + (1 - first) * 32, 32)], r1.at[j], s1s.at[j], s1r.at[j], along_first)

    def s2(j):
        return remote(part.at[j, pl.ds(quarter + (1 - second) * 16, 16)], r2.at[j], s2s.at[j], s2r.at[j], along_second)

    def g1(j):
        piece = out_ref.at[pl.ds(eighth, 16), cols(j)]
        return remote(piece, piece, g1s.at[j], g1r.at[j], along_second)

    def g2(j):
        piece = out_ref.at[pl.ds(quarter, 32), cols(j)]
        return remote(piece, piece, g2s.at[j], g2r.at[j], along_first)

    def g3(j):
        piece = out_ref.at[pl.ds(half, 64), cols(j)]
        return remote(piece, piece, g3s.at[j], g3r.at[j], partner)

    def arrived(ref, sem):
        pltpu.make_async_copy(ref, ref, sem).wait()

    def at(t, lag, body):
        j = t - lag

        @pl.when(jnp.logical_and(j >= 0, j < chunks))
        def _():
            body(j)

    def stage5(j):
        arrived(out_ref.at[pl.ds(core * 64 + (1 - first) * 32, 32), cols(j)], g2r.at[j])
        g3(j).start()

    def stage4(j):
        arrived(out_ref.at[pl.ds(quarter + (1 - second) * 16, 16), cols(j)], g1r.at[j])
        g2(j).start()

    def stage3(j):
        arrived(r2.at[j], s2r.at[j])
        total = part[j, pl.ds(pl.multiple_of(eighth, 16), 16)] + r2[j]
        out_ref[pl.ds(pl.multiple_of(eighth, 16), 16), cols(j)] = (xrows[:, cols(j)].astype(F32) + total).astype(BF16)
        g1(j).start()

    def stage2(j):
        arrived(r1.at[j], s1r.at[j])
        part[j, pl.ds(pl.multiple_of(quarter, 16), 32)] += r1[j]
        s2(j).start()

    def stage1(j):
        arrived(r0.at[j], s0r.at[j])
        part[j, pl.ds(pl.multiple_of(half, 16), 64)] += r0[j]
        s1(j).start()

    def stage0(j):
        w_copy(j).wait()
        part[j] = jnp.dot(o_all[...], wbuf[j % slots], preferred_element_type=F32)

        @pl.when(j + slots < chunks)
        def _():
            w_copy(j + slots).start()
        s0(j).start()

    @pl.loop(0, chunks + LAGS[-1])
    def _(t):
        at(t, 0, stage0)
        at(t, LAGS[0], stage1)
        at(t, LAGS[1], stage2)
        at(t, LAGS[2], stage3)
        at(t, LAGS[3], stage4)
        at(t, LAGS[4], stage5)

    for offset in range(1, 8):
        o_copy(offset).wait_send()

    @pl.loop(0, chunks)
    def _(j):
        arrived(out_ref.at[pl.ds((1 - core) * 64, 64), cols(j)], g3r.at[j])
        for copy in (s0, s1, s2, g1, g2, g3):
            copy(j).wait_send()


def mix(attended, w_out, tokens):
    depth, width = w_out.shape
    chunk, slots = 512, 8
    chunks = width // chunk
    vmem = pl.BlockSpec(memory_space=pltpu.VMEM)
    hbm = pl.BlockSpec(memory_space=pltpu.HBM)
    sems = pltpu.SemaphoreType.DMA((chunks,))
    return pl.pallas_call(
        functools.partial(mix_kernel, chunk, slots),
        out_shape=jax.ShapeDtypeStruct((128, width), BF16),
        in_specs=[vmem, hbm, hbm],
        out_specs=vmem,
        scratch_shapes=[
            pltpu.VMEM((128, depth), BF16),
            pltpu.VMEM((slots, depth, chunk), BF16),
            pltpu.VMEM((16, width), BF16),
            pltpu.VMEM((chunks, 128, chunk), F32),
            pltpu.VMEM((chunks, 64, chunk), F32),
            pltpu.VMEM((chunks, 32, chunk), F32),
            pltpu.VMEM((chunks, 16, chunk), F32),
            pltpu.SemaphoreType.DMA((slots,)),
            pltpu.SemaphoreType.DMA,
            pltpu.SemaphoreType.DMA((8,)),
            pltpu.SemaphoreType.DMA((8,)),
        ] + [sems] * 12,
        compiler_params=pltpu.CompilerParams(collective_id=1, has_side_effects=True, vmem_limit_bytes=42 * MIB),
        cost_estimate=pl.CostEstimate(flops=2 * 128 * depth * width, bytes_accessed=depth * width * 2, transcendentals=0),
        name="mix",
    )(attended, *(pltpu.with_memory_space_constraint(a, pltpu.HBM) for a in (w_out, tokens)))


def solution(mesh):
    def local_step(tokens, w_query, w_key, w_value, w_out, key_cache, value_cache, lengths):
        queries, key_new, value_new = project_queries(tokens, w_query, w_key, w_value)
        attended, key_new, value_new = attend(lengths, queries, key_new, value_new, key_cache, value_cache)
        out_tokens = mix(attended, w_out, tokens)
        return (out_tokens, key_new.reshape(32, 1, 256), value_new.reshape(32, 1, 256))

    cache_spec = P(("replica", "model"), None, None, None)
    new_spec = P(("replica", "model"), None, None)
    return jax.shard_map(
        local_step,
        mesh=mesh,
        in_specs=(P("replica", None), P(None, ("heads", "model")), P(None, None), P(None, None), P(("heads", "model"), None), cache_spec, cache_spec, P(("replica", "model"))),
        out_specs=(P("replica", None), new_spec, new_spec),
        check_vma=False,
    )
```

```python
import functools

import jax
import jax.numpy as jnp
from jax import lax
from jax.experimental import pallas as pl
from jax.experimental.pallas import tpu as pltpu
from jax.sharding import PartitionSpec as P

MESH = pl.DeviceIdType.MESH
F32 = jnp.float32
BF16 = jnp.bfloat16
MIB = 1 << 20


def coordinates():
    y = lax.axis_index("heads")
    model = lax.axis_index("model")
    return y, model, model // 2, model % 2


def greet(others):
    y, model, _, _ = coordinates()
    me = y * 4 + model
    barrier = pltpu.get_barrier_semaphore()
    for offset in others:
        peer = (me + offset) % 8
        pl.semaphore_signal(barrier, inc=1, device_id={"heads": peer // 4, "model": peer % 4}, device_id_type=MESH)


def query_kernel(groups, cols, depth, slots, kv_depth, x_ref, wq_ref, wk_ref, wv_ref, q_ref, kn_ref, vn_ref, perm, back, xbuf, wbuf, kvbuf, acc, kvacc, qs, kvs, kv_all,
                 x_sem, w_sem, kv_sem, q_send, q_recv, kv_send, kv_recv, self_sem, kv_self_sem):
    y, model, _, _ = coordinates()
    me = y * 4 + model
    width = x_ref.shape[1]
    steps = width // depth
    kv_steps = width // kv_depth
    total = groups * steps

    def w_copy(i):
        g, k = i // steps, i % steps
        return pltpu.make_async_copy(wq_ref.at[pl.ds(k * depth, depth), pl.ds(g * cols, cols)], wbuf.at[i % slots], w_sem.at[i % slots])

    def x_copy(k):
        part = pl.ds(pl.multiple_of(k * depth, 128), depth)
        return pltpu.make_async_copy(x_ref.at[:, part], xbuf.at[:, part], x_sem.at[k])

    def kv_copy(ref, col, k):
        return pltpu.make_async_copy(ref.at[pl.ds(k * kv_depth, kv_depth), pl.ds(col * 128, 128)], kvbuf.at[k], kv_sem.at[k])

    for i in range(max(steps, slots)):
        if i < steps:
            x_copy(i).start()
        if i < slots:
            w_copy(i).start()

    greet(range(1, 8))
    column = lax.broadcasted_iota(jnp.int32, (48, 768), 1)
    row = lax.broadcasted_iota(jnp.int32, (48, 768), 0)
    for n in range(16):
        perm[n * 48:(n + 1) * 48] = jnp.where(column == row * 16 + n, 1.0, 0.0).astype(BF16)
        back[n * 48:(n + 1) * 48] = jnp.where(column == row % 16 * 48 + row // 16 + 3 * n, 1.0, 0.0).astype(BF16)
    pl.semaphore_wait(pltpu.get_barrier_semaphore(), 7)

    per_group = cols // 256

    def q_copy(g, h, offset):
        head = g * per_group + h
        peer = (me + offset) % 8
        rows = (peer % 4) * 2 + peer // 4
        return pltpu.make_async_remote_copy(
            src_ref=qs.at[head, pl.ds(rows * 16, 16)], dst_ref=q_ref.at[me * 6 + head],
            send_sem=q_send, recv_sem=q_recv,
            device_id={"heads": peer // 4, "model": peer % 4}, device_id_type=MESH)

    def q_self(head):
        return pltpu.make_async_copy(qs.at[head, pl.ds((model * 2 + y) * 16, 16)], q_ref.at[me * 6 + head], self_sem)

    @pl.loop(0, total)
    def _(i):
        g, k = i // steps, i % steps

        @pl.when(i < steps)
        def _():
            x_copy(i).wait()

        w_copy(i).wait()
        part = jnp.dot(xbuf[:, pl.ds(pl.multiple_of(k * depth, 128), depth)], wbuf[i % slots], preferred_element_type=F32)

        @pl.when(k == 0)
        def _():
            acc[...] = part

        @pl.when(k > 0)
        def _():
            acc[...] += part

        @pl.when(i + slots < total)
        def _():
            w_copy(i + slots).start()

        for n in range(kv_steps):
            @pl.when(i == total - kv_steps + n - 1)
            def _():
                @pl.when(model < 2)
                def _():
                    kv_copy(wk_ref, model % 2, n).start()

                @pl.when(model >= 2)
                def _():
                    kv_copy(wv_ref, model % 2, n).start()

        @pl.when(k == steps - 1)
        def _():
            for h in range(per_group):
                qs[g * per_group + h] = acc[:, h * 256:(h + 1) * 256].astype(BF16)
            for h in range(per_group):
                for offset in (7, 6, 5, 4, 3, 2, 1):
                    q_copy(g, h, offset).start()
                q_self(g * per_group + h).start()

    kvacc[...] = jnp.zeros_like(kvacc)

    @pl.loop(0, kv_steps)
    def _(k):
        kv_copy(wk_ref, 0, k).wait()
        kvacc[...] += jnp.dot(xbuf[:, pl.ds(pl.multiple_of(k * kv_depth, 128), kv_depth)], kvbuf[k], preferred_element_type=F32)

    kvs[...] = kvacc[...].astype(BF16)

    def kv_send_copy(offset):
        peer = (model + offset) % 4
        return pltpu.make_async_remote_copy(
            src_ref=kvs.at[pl.ds(peer * 32, 32)], dst_ref=kv_all.at[model], send_sem=kv_send, recv_sem=kv_recv,
            device_id={"heads": y, "model": peer}, device_id_type=MESH)

    for offset in (2, 3, 1):
        kv_send_copy(offset).start()
    kv_self = pltpu.make_async_copy(kvs.at[pl.ds(model * 32, 32)], kv_all.at[model], kv_self_sem)
    kv_self.start()

    def settle(ref, sem):
        pltpu.make_async_copy(ref, ref, sem).wait()

    settle(q_ref.at[pl.ds(0, 6)], self_sem)
    settle(q_ref.at[pl.ds(0, 42)], q_send)
    settle(q_ref.at[pl.ds(0, 42)], q_recv)
    kv_self.wait()
    settle(kv_all.at[pl.ds(0, 3)], kv_send)
    settle(kv_all.at[pl.ds(0, 3)], kv_recv)
    kn_ref[:, :128] = kv_all[0]
    kn_ref[:, 128:] = kv_all[1]
    vn_ref[:, :128] = kv_all[2]
    vn_ref[:, 128:] = kv_all[3]


def project_queries(tokens, w_query, w_key, w_value):
    rows, width = tokens.shape
    groups, cols, depth, slots = 6, 256, 4608, 6
    kv_depth = 4608
    vmem = pl.BlockSpec(memory_space=pltpu.VMEM)
    hbm = pl.BlockSpec(memory_space=pltpu.HBM)
    return pl.pallas_call(
        functools.partial(query_kernel, groups, cols, depth, slots, kv_depth),
        out_shape=(jax.ShapeDtypeStruct((48, 16, 256), BF16), jax.ShapeDtypeStruct((32, 256), BF16), jax.ShapeDtypeStruct((32, 256), BF16),
                   jax.ShapeDtypeStruct((768, 768), BF16), jax.ShapeDtypeStruct((768, 768), BF16)),
        in_specs=[hbm, hbm, hbm, hbm],
        out_specs=(vmem,) * 5,
        scratch_shapes=[
            pltpu.VMEM((rows, width), BF16),
            pltpu.VMEM((slots, depth, cols), BF16),
            pltpu.VMEM((width // kv_depth, kv_depth, 128), BF16),
            pltpu.VMEM((rows, cols), F32),
            pltpu.VMEM((rows, 128), F32),
            pltpu.VMEM((6, rows, 256), BF16),
            pltpu.VMEM((rows, 128), BF16),
            pltpu.VMEM((4, 32, 128), BF16),
            pltpu.SemaphoreType.DMA((width // depth,)),
            pltpu.SemaphoreType.DMA((slots,)),
            pltpu.SemaphoreType.DMA((width // kv_depth,)),
        ] + [pltpu.SemaphoreType.DMA] * 6,
        compiler_params=pltpu.CompilerParams(collective_id=0, has_side_effects=True, vmem_limit_bytes=48 * MIB),
        cost_estimate=pl.CostEstimate(flops=2 * rows * width * 1664, bytes_accessed=width * 1664 * 2, transcendentals=0),
        name="query",
    )(*(pltpu.with_memory_space_constraint(a, pltpu.HBM) for a in (tokens, w_query, w_key, w_value)))


ITEM = 1024


def attend_kernel(slots, len_ref, q_ref, kn_ref, vn_ref, perm, back, key_ref, value_ref, o_ref, kn_out, vn_out, kbuf, vbuf, qs, os, sn, vnf, sbuf, pbuf, acc, m_ref, l_ref, a_ref, r_ref, items, left, k_sem, v_sem):
    y = lax.axis_index("heads")
    first_seq = y * 16
    power = 256 ** -0.5 * 1.4426950408889634

    def list_seq(s, count):
        length = len_ref[first_seq + s]
        chunks = (length + ITEM - 1) // ITEM
        for c in range(4):
            @pl.when(c < chunks)
            def _():
                items[count + c] = s * 4 + c
                left[count + c] = length - c * ITEM
        return count + chunks

    total = lax.fori_loop(0, 16, list_seq, jnp.int32(0))
    items[total] = items[total - 1] // 4 * 4 + 3
    left[total] = 0
    pairs = (total + 1) // 2

    def copy(i, ref, buf, sem, whole=False):
        entry = items[i]
        slot = i % slots
        size = pl.multiple_of((jnp.where(whole, ITEM, jnp.minimum(left[i], ITEM)) + 15) // 16 * 16, 16)
        return pltpu.make_async_copy(ref.at[first_seq + entry // 4, 0, pl.ds(pl.multiple_of(entry % 4 * ITEM, ITEM), size)], buf.at[slot, pl.ds(0, size)], sem.at[slot])

    def k_copy(i):
        return copy(i, key_ref, kbuf, k_sem)

    def v_copy(i):
        return copy(i, value_ref, vbuf, v_sem, i < slots)

    for i in range(slots - 2):
        @pl.when(i < total)
        def _():
            k_copy(i).start()
            v_copy(i).start()

    kn_out[...] = kn_ref[...]
    vn_out[...] = vn_ref[...]
    qs[...] = jnp.dot(perm[...], q_ref[...].reshape(768, 256), preferred_element_type=F32).astype(BF16)
    vnf[...] = vn_ref[pl.ds(pl.multiple_of(first_seq, 16), 16), :].astype(F32)
    knf = kn_ref[pl.ds(pl.multiple_of(first_seq, 16), 16), :].astype(F32)
    for n in range(16):
        rows = slice(n * 48, (n + 1) * 48)
        sn[rows] = jnp.broadcast_to(jnp.sum(qs[rows].astype(F32) * knf[n:n + 1], axis=1, keepdims=True), (48, 128))
    m_ref[...] = jnp.zeros_like(m_ref)
    l_ref[...] = jnp.ones_like(l_ref)
    acc[...] = jnp.zeros_like(acc)

    def rows_of(entry):
        return pl.ds(pl.multiple_of(entry // 4 * 48, 16), 48)

    def score(i):
        return lax.dot_general(qs[rows_of(items[i]), :], kbuf[i % slots], (((1,), (1,)), ((), ())), preferred_element_type=F32)

    lane = lax.broadcasted_iota(jnp.int32, (48, 128), 1)

    halves = (slice(0, 128), slice(128, 256))
    chunks = [slice(n * 128, (n + 1) * 128) for n in range(ITEM // 128)]

    def pair_scores(pair, turn):
        for n in range(2):
            sbuf[turn, n] = score(2 * pair + n)

    def weigh(pair, turn):
        m, l = m_ref[...], l_ref[...]
        for n in range(2):
            i = 2 * pair + n
            entry = items[i]
            fresh = entry % 4 == 0
            m_old = jnp.where(fresh, sn[rows_of(entry), :], m)
            x = [jnp.where(lane < left[i] - c.start, sbuf[turn, n, :, c], -jnp.inf) for c in chunks]
            top = functools.reduce(jnp.maximum, x)
            m = jnp.maximum(m_old, jnp.broadcast_to(jnp.max(top, axis=1, keepdims=True), (48, 128)))
            alpha = jnp.exp2((m_old - m) * power)
            p = [jnp.exp2((v - m) * power) for v in x]
            l = jnp.where(fresh, 1.0, l) * alpha + jnp.broadcast_to(jnp.sum(functools.reduce(jnp.add, p), axis=1, keepdims=True), (48, 128))
            a_ref[turn, n] = alpha
            r_ref[turn, n] = l
            for c, v in zip(chunks, p):
                pbuf[turn, n, :, c] = v.astype(BF16)
        m_ref[...] = m
        l_ref[...] = l

    def blend(pair, turn):
        for n in range(2):
            i = 2 * pair + n
            entry = items[i]
            added = jnp.dot(pbuf[turn, n], vbuf[i % slots], preferred_element_type=F32)
            alpha = a_ref[turn, n]
            inverse = 1.0 / r_ref[turn, n]
            fresh_row = vnf[pl.ds(entry // 4, 1), :]
            for h in halves:
                now = jnp.where(entry % 4 == 0, jnp.broadcast_to(fresh_row[:, h], (48, 128)), acc[:, h]) * alpha + added[:, h]
                acc[:, h] = now
                os[rows_of(entry), h] = (now * inverse).astype(BF16)

    def arrive(copy, pair):
        for n in range(2):
            @pl.when(2 * pair + n < total)
            def _():
                copy(2 * pair + n).wait()

    arrive(k_copy, 0)
    pair_scores(0, 0)
    weigh(0, 0)
    arrive(k_copy, 1)
    pair_scores(jnp.minimum(1, pairs - 1), 1)

    @pl.loop(0, pairs)
    def _(pair):
        for n in range(2):
            i = 2 * pair + slots - 2 + n

            @pl.when(i < total)
            def _():
                k_copy(i).start()
                v_copy(i).start()

        arrive(k_copy, pair + 2)
        arrive(v_copy, pair)
        turn = pair % 2
        blend(pair, turn)
        weigh(jnp.minimum(pair + 1, pairs - 1), 1 - turn)
        pair_scores(jnp.minimum(pair + 2, pairs - 1), turn)

    mixed = jnp.dot(back[...], os[...], preferred_element_type=F32).astype(BF16)
    for h in range(48):
        o_ref[h // 6, :, (h % 6) * 256:(h % 6 + 1) * 256] = mixed[h * 16:(h + 1) * 16]


def attend(lengths, queries, key_new, value_new, perm, back, key_cache, value_cache):
    slots = 12
    vmem = pl.BlockSpec(memory_space=pltpu.VMEM)
    hbm = pl.BlockSpec(memory_space=pltpu.HBM)
    return pl.pallas_call(
        functools.partial(attend_kernel, slots),
        out_shape=(jax.ShapeDtypeStruct((8, 16, 1536), BF16), jax.ShapeDtypeStruct((32, 256), BF16), jax.ShapeDtypeStruct((32, 256), BF16)),
        in_specs=[pl.BlockSpec(memory_space=pltpu.SMEM), vmem, vmem, vmem, vmem, vmem, hbm, hbm],
        out_specs=(vmem, vmem, vmem),
        scratch_shapes=[
            pltpu.VMEM((slots, ITEM, 256), BF16),
            pltpu.VMEM((slots, ITEM, 256), BF16),
            pltpu.VMEM((768, 256), BF16),
            pltpu.VMEM((768, 256), BF16),
            pltpu.VMEM((768, 128), F32),
            pltpu.VMEM((16, 256), F32),
            pltpu.VMEM((2, 2, 48, ITEM), F32),
            pltpu.VMEM((2, 2, 48, ITEM), BF16),
            pltpu.VMEM((48, 256), F32),
            pltpu.VMEM((48, 128), F32),
            pltpu.VMEM((48, 128), F32),
            pltpu.VMEM((2, 2, 48, 128), F32),
            pltpu.VMEM((2, 2, 48, 128), F32),
            pltpu.SMEM((72,), jnp.int32),
            pltpu.SMEM((72,), jnp.int32),
            pltpu.SemaphoreType.DMA((slots,)),
            pltpu.SemaphoreType.DMA((slots,)),
        ],
        compiler_params=pltpu.CompilerParams(vmem_limit_bytes=40 * MIB),
        cost_estimate=pl.CostEstimate(flops=4 * 16 * 48 * 2048 * 256, bytes_accessed=16 * 2048 * 1024, transcendentals=16 * 48 * 2048),
        name="attend",
    )(lengths, queries, key_new, value_new, perm, back, key_cache, value_cache)


LAGS = (2, 5, 9, 12, 15)


def mix_kernel(chunk, slots, o_ref, w_ref, x_ref, out_ref, o_all, wbuf, xrows, part, r0, r1, r2,
               w_sem, x_sem, o_send, o_recv, o_self_sem, s0s, s1s, s2s, g1s, g2s, g3s, g3r, s0r, s1r, s2r, g1r, g2r):
    y, model, x, core = coordinates()
    me = y * 4 + model
    width = w_ref.shape[1]
    chunks = width // chunk
    first, second = x * (1 - core) + y * core, y * (1 - core) + x * core
    own = core * 4 + first * 2 + second
    flip_x = {"heads": y, "model": (1 - x) * 2 + core}
    partner = {"heads": y, "model": x * 2 + 1 - core}
    along_first = {"heads": y * (1 - core) + (1 - y) * core, "model": ((1 - x) * (1 - core) + x * core) * 2 + core}
    along_second = {"heads": (1 - y) * (1 - core) + y * core, "model": (x * (1 - core) + (1 - x) * core) * 2 + core}

    def w_copy(t):
        return pltpu.make_async_copy(w_ref.at[:, pl.ds(pl.multiple_of(t * chunk, chunk), chunk)], wbuf.at[t % slots], w_sem.at[t % slots])

    for t in range(slots):
        w_copy(t).start()
    x_copy = pltpu.make_async_copy(x_ref.at[pl.ds(own * 16, 16)], xrows, x_sem)
    x_copy.start()

    greet(range(1, 8))
    pl.semaphore_wait(pltpu.get_barrier_semaphore(), 7)

    mine = model * 2 + y

    def o_copy(offset):
        peer = (me + offset) % 8
        return pltpu.make_async_remote_copy(
            src_ref=o_ref.at[peer], dst_ref=o_all.at[pl.ds(mine * 16, 16)], send_sem=o_send, recv_sem=o_recv,
            device_id={"heads": peer // 4, "model": peer % 4}, device_id_type=MESH)

    for offset in range(1, 8):
        o_copy(offset).start()
    o_self = pltpu.make_async_copy(o_ref.at[me], o_all.at[pl.ds(mine * 16, 16)], o_self_sem)
    o_self.start()
    o_self.wait()
    pltpu.make_async_copy(o_all.at[pl.ds(0, 112)], o_all.at[pl.ds(0, 112)], o_recv).wait()
    x_copy.wait()

    def remote(src, dst, send, recv, device):
        return pltpu.make_async_remote_copy(src_ref=src, dst_ref=dst, send_sem=send, recv_sem=recv, device_id=device, device_id_type=MESH)

    half, quarter = core * 64, core * 64 + first * 32
    eighth = quarter + second * 16
    cols = lambda j: pl.ds(pl.multiple_of(j * chunk, chunk), chunk)

    def s0(j):
        return remote(part.at[j, pl.ds((1 - core) * 64, 64)], r0.at[j], s0s, s0r.at[j], partner)

    def s1(j):
        return remote(part.at[j, pl.ds(half + (1 - first) * 32, 32)], r1.at[j], s1s, s1r.at[j], along_first)

    def s2(j):
        return remote(part.at[j, pl.ds(quarter + (1 - second) * 16, 16)], r2.at[j], s2s, s2r.at[j], along_second)

    def g1(j):
        piece = out_ref.at[pl.ds(eighth, 16), cols(j)]
        return remote(piece, piece, g1s, g1r.at[j], along_second)

    def g2(j):
        piece = out_ref.at[pl.ds(quarter, 32), cols(j)]
        return remote(piece, piece, g2s, g2r.at[j], along_first)

    def g3(j):
        piece = out_ref.at[pl.ds(half, 64), cols(j)]
        return remote(piece, piece, g3s, g3r, partner)

    def arrived(ref, sem):
        pltpu.make_async_copy(ref, ref, sem).wait()

    def at(t, lag, body):
        j = t - lag

        @pl.when(jnp.logical_and(j >= 0, j < chunks))
        def _():
            body(j)

    def stage5(j):
        arrived(out_ref.at[pl.ds(core * 64 + (1 - first) * 32, 32), cols(j)], g2r.at[j])
        g3(j).start()

    def stage4(j):
        arrived(out_ref.at[pl.ds(quarter + (1 - second) * 16, 16), cols(j)], g1r.at[j])
        g2(j).start()

    def stage3(j):
        arrived(r2.at[j], s2r.at[j])
        total = part[j, pl.ds(pl.multiple_of(eighth, 16), 16)] + r2[j]
        out_ref[pl.ds(pl.multiple_of(eighth, 16), 16), cols(j)] = (xrows[:, cols(j)].astype(F32) + total).astype(BF16)
        g1(j).start()

    def stage2(j):
        arrived(r1.at[j], s1r.at[j])
        part[j, pl.ds(pl.multiple_of(quarter, 16), 32)] += r1[j]
        s2(j).start()

    def stage1(j):
        arrived(r0.at[j], s0r.at[j])
        part[j, pl.ds(pl.multiple_of(half, 16), 64)] += r0[j]
        s1(j).start()

    def stage0(j):
        w_copy(j).wait()
        part[j] = jnp.dot(o_all[...], wbuf[j % slots], preferred_element_type=F32)

        @pl.when(j + slots < chunks)
        def _():
            w_copy(j + slots).start()
        s0(j).start()

    @pl.loop(0, chunks + LAGS[-1])
    def _(t):
        at(t, 0, stage0)
        at(t, LAGS[0], stage1)
        at(t, LAGS[1], stage2)
        at(t, LAGS[2], stage3)
        at(t, LAGS[3], stage4)
        at(t, LAGS[4], stage5)

    arrived(o_ref.at[pl.ds(0, 7)], o_send)
    arrived(out_ref.at[pl.ds(0, 64)], g3r)
    for ref, sem in ((r0, s0s), (r1, s1s), (r2, s2s), (out_ref.at[pl.ds(0, 16)], g1s), (out_ref.at[pl.ds(0, 32)], g2s), (out_ref.at[pl.ds(0, 64)], g3s)):
        arrived(ref, sem)


def mix(attended, w_out, tokens):
    depth, width = w_out.shape
    chunk, slots = 1024, 4
    chunks = width // chunk
    vmem = pl.BlockSpec(memory_space=pltpu.VMEM)
    hbm = pl.BlockSpec(memory_space=pltpu.HBM)
    sems = pltpu.SemaphoreType.DMA((chunks,))
    return pl.pallas_call(
        functools.partial(mix_kernel, chunk, slots),
        out_shape=jax.ShapeDtypeStruct((128, width), BF16),
        in_specs=[vmem, hbm, hbm],
        out_specs=vmem,
        scratch_shapes=[
            pltpu.VMEM((128, depth), BF16),
            pltpu.VMEM((slots, depth, chunk), BF16),
            pltpu.VMEM((16, width), BF16),
            pltpu.VMEM((chunks, 128, chunk), F32),
            pltpu.VMEM((chunks, 64, chunk), F32),
            pltpu.VMEM((chunks, 32, chunk), F32),
            pltpu.VMEM((chunks, 16, chunk), F32),
            pltpu.SemaphoreType.DMA((slots,)),
        ] + [pltpu.SemaphoreType.DMA] * 11 + [sems] * 5,
        compiler_params=pltpu.CompilerParams(collective_id=1, has_side_effects=True, vmem_limit_bytes=42 * MIB),
        cost_estimate=pl.CostEstimate(flops=2 * 128 * depth * width, bytes_accessed=depth * width * 2, transcendentals=0),
        name="mix",
    )(attended, *(pltpu.with_memory_space_constraint(a, pltpu.HBM) for a in (w_out, tokens)))


def solution(mesh):
    def local_step(tokens, w_query, w_key, w_value, w_out, key_cache, value_cache, lengths):
        queries, key_new, value_new, perm, back = project_queries(tokens, w_query, w_key, w_value)
        attended, key_new, value_new = attend(lengths, queries, key_new, value_new, perm, back, key_cache, value_cache)
        out_tokens = mix(attended, w_out, tokens)
        return (out_tokens, key_new.reshape(32, 1, 256), value_new.reshape(32, 1, 256))

    cache_spec = P(("replica", "model"), None, None, None)
    new_spec = P(("replica", "model"), None, None)
    return jax.shard_map(
        local_step,
        mesh=mesh,
        in_specs=(P("replica", None), P(None, ("heads", "model")), P(None, None), P(None, None), P(("heads", "model"), None), cache_spec, cache_spec, P(("replica", "model"))),
        out_specs=(P("replica", None), new_spec, new_spec),
        check_vma=False,
    )
```

```python
import functools

import jax
import jax.numpy as jnp
from jax import lax
from jax.experimental import pallas as pl
from jax.experimental.pallas import tpu as pltpu
from jax.sharding import PartitionSpec as P

MESH = pl.DeviceIdType.MESH
F32 = jnp.float32
BF16 = jnp.bfloat16
MIB = 1 << 20


def coordinates():
    y = lax.axis_index("heads")
    model = lax.axis_index("model")
    return y, model, model // 2, model % 2


def greet(others):
    y, model, _, _ = coordinates()
    me = y * 4 + model
    barrier = pltpu.get_barrier_semaphore()
    for offset in others:
        peer = (me + offset) % 8
        pl.semaphore_signal(barrier, inc=1, device_id={"heads": peer // 4, "model": peer % 4}, device_id_type=MESH)


def query_kernel(groups, cols, depth, slots, kv_depth, x_ref, wq_ref, wk_ref, wv_ref, q_ref, kn_ref, vn_ref, perm, back, xbuf, wbuf, kvbuf, acc, kvacc, qs, kvs, kv_all,
                 x_sem, w_sem, kv_sem, q_send, q_recv, kv_send, kv_recv, self_sem, kv_self_sem):
    y, model, _, _ = coordinates()
    me = y * 4 + model
    width = x_ref.shape[1]
    steps = width // depth
    kv_steps = width // kv_depth
    total = groups * steps

    def w_copy(i):
        g, k = i // steps, i % steps
        return pltpu.make_async_copy(wq_ref.at[pl.ds(k * depth, depth), pl.ds(g * cols, cols)], wbuf.at[i % slots], w_sem.at[i % slots])

    def x_copy(k):
        part = pl.ds(pl.multiple_of(k * depth, 128), depth)
        return pltpu.make_async_copy(x_ref.at[:, part], xbuf.at[:, part], x_sem.at[k])

    def kv_copy(ref, col, k):
        return pltpu.make_async_copy(ref.at[pl.ds(k * kv_depth, kv_depth), pl.ds(col * 128, 128)], kvbuf.at[k], kv_sem.at[k])

    for i in range(max(steps, slots)):
        if i < steps:
            x_copy(i).start()
        if i < slots:
            w_copy(i).start()

    greet(range(1, 8))
    column = lax.broadcasted_iota(jnp.int32, (48, 768), 1)
    row = lax.broadcasted_iota(jnp.int32, (48, 768), 0)
    for n in range(16):
        perm[n * 48:(n + 1) * 48] = jnp.where(column == row * 16 + n, 1.0, 0.0).astype(BF16)
        back[n * 48:(n + 1) * 48] = jnp.where(column == row % 16 * 48 + row // 16 + 3 * n, 1.0, 0.0).astype(BF16)
    pl.semaphore_wait(pltpu.get_barrier_semaphore(), 7)

    per_group = cols // 256

    def q_copy(g, h, offset):
        head = g * per_group + h
        peer = (me + offset) % 8
        rows = (peer % 4) * 2 + peer // 4
        return pltpu.make_async_remote_copy(
            src_ref=qs.at[head, pl.ds(rows * 16, 16)], dst_ref=q_ref.at[me * 6 + head],
            send_sem=q_send, recv_sem=q_recv,
            device_id={"heads": peer // 4, "model": peer % 4}, device_id_type=MESH)

    def q_self(head):
        return pltpu.make_async_copy(qs.at[head, pl.ds((model * 2 + y) * 16, 16)], q_ref.at[me * 6 + head], self_sem)

    @pl.loop(0, total)
    def _(i):
        g, k = i // steps, i % steps

        @pl.when(i < steps)
        def _():
            x_copy(i).wait()

        w_copy(i).wait()
        part = jnp.dot(xbuf[:, pl.ds(pl.multiple_of(k * depth, 128), depth)], wbuf[i % slots], preferred_element_type=F32)

        @pl.when(k == 0)
        def _():
            acc[...] = part

        @pl.when(k > 0)
        def _():
            acc[...] += part

        @pl.when(i + slots < total)
        def _():
            w_copy(i + slots).start()

        for n in range(kv_steps):
            @pl.when(i == total - kv_steps + n - 1)
            def _():
                @pl.when(model < 2)
                def _():
                    kv_copy(wk_ref, model % 2, n).start()

                @pl.when(model >= 2)
                def _():
                    kv_copy(wv_ref, model % 2, n).start()

        @pl.when(k == steps - 1)
        def _():
            for h in range(per_group):
                qs[g * per_group + h] = acc[:, h * 256:(h + 1) * 256].astype(BF16)
            for h in range(per_group):
                for offset in (7, 6, 5, 4, 3, 2, 1):
                    q_copy(g, h, offset).start()
                q_self(g * per_group + h).start()

    kvacc[...] = jnp.zeros_like(kvacc)

    @pl.loop(0, kv_steps)
    def _(k):
        kv_copy(wk_ref, 0, k).wait()
        kvacc[...] += jnp.dot(xbuf[:, pl.ds(pl.multiple_of(k * kv_depth, 128), kv_depth)], kvbuf[k], preferred_element_type=F32)

    kvs[...] = kvacc[...].astype(BF16)

    def kv_send_copy(offset):
        peer = (model + offset) % 4
        return pltpu.make_async_remote_copy(
            src_ref=kvs.at[pl.ds(peer * 32, 32)], dst_ref=kv_all.at[model], send_sem=kv_send, recv_sem=kv_recv,
            device_id={"heads": y, "model": peer}, device_id_type=MESH)

    for offset in (2, 3, 1):
        kv_send_copy(offset).start()
    kv_self = pltpu.make_async_copy(kvs.at[pl.ds(model * 32, 32)], kv_all.at[model], kv_self_sem)
    kv_self.start()

    def settle(ref, sem):
        pltpu.make_async_copy(ref, ref, sem).wait()

    settle(q_ref.at[pl.ds(0, 6)], self_sem)
    settle(q_ref.at[pl.ds(0, 42)], q_send)
    settle(q_ref.at[pl.ds(0, 42)], q_recv)
    kv_self.wait()
    settle(kv_all.at[pl.ds(0, 3)], kv_send)
    settle(kv_all.at[pl.ds(0, 3)], kv_recv)
    kn_ref[:, :128] = kv_all[0]
    kn_ref[:, 128:] = kv_all[1]
    vn_ref[:, :128] = kv_all[2]
    vn_ref[:, 128:] = kv_all[3]


def project_queries(tokens, w_query, w_key, w_value):
    rows, width = tokens.shape
    groups, cols, depth, slots = 6, 256, 4608, 6
    kv_depth = 4608
    vmem = pl.BlockSpec(memory_space=pltpu.VMEM)
    hbm = pl.BlockSpec(memory_space=pltpu.HBM)
    return pl.pallas_call(
        functools.partial(query_kernel, groups, cols, depth, slots, kv_depth),
        out_shape=(jax.ShapeDtypeStruct((48, 16, 256), BF16), jax.ShapeDtypeStruct((32, 256), BF16), jax.ShapeDtypeStruct((32, 256), BF16),
                   jax.ShapeDtypeStruct((768, 768), BF16), jax.ShapeDtypeStruct((768, 768), BF16)),
        in_specs=[hbm, hbm, hbm, hbm],
        out_specs=(vmem,) * 5,
        scratch_shapes=[
            pltpu.VMEM((rows, width), BF16),
            pltpu.VMEM((slots, depth, cols), BF16),
            pltpu.VMEM((width // kv_depth, kv_depth, 128), BF16),
            pltpu.VMEM((rows, cols), F32),
            pltpu.VMEM((rows, 128), F32),
            pltpu.VMEM((6, rows, 256), BF16),
            pltpu.VMEM((rows, 128), BF16),
            pltpu.VMEM((4, 32, 128), BF16),
            pltpu.SemaphoreType.DMA((width // depth,)),
            pltpu.SemaphoreType.DMA((slots,)),
            pltpu.SemaphoreType.DMA((width // kv_depth,)),
        ] + [pltpu.SemaphoreType.DMA] * 6,
        compiler_params=pltpu.CompilerParams(collective_id=0, has_side_effects=True, vmem_limit_bytes=48 * MIB),
        cost_estimate=pl.CostEstimate(flops=2 * rows * width * 1664, bytes_accessed=width * 1664 * 2, transcendentals=0),
        name="query",
    )(*(pltpu.with_memory_space_constraint(a, pltpu.HBM) for a in (tokens, w_query, w_key, w_value)))


ITEM = 1024


def attend_kernel(slots, len_ref, q_ref, kn_ref, vn_ref, perm, back, key_ref, value_ref, o_ref, kn_out, vn_out, kbuf, vbuf, qs, os, sn, vnf, sbuf, pbuf, acc, m_ref, l_ref, a_ref, r_ref, items, left, sizes, k_sem, v_sem):
    y = lax.axis_index("heads")
    first_seq = y * 16
    power = 256 ** -0.5 * 1.4426950408889634

    def list_seq(s, count):
        length = len_ref[first_seq + s]
        chunks = (length + ITEM - 1) >> 10
        for c in range(4):
            @pl.when(c < chunks)
            def _():
                items[count + c] = s * 4 + c
                left[count + c] = length - c * ITEM
                sizes[count + c] = jnp.minimum((length - c * ITEM + 15) & ~15, ITEM)
        return count + chunks

    total = lax.fori_loop(0, 16, list_seq, jnp.int32(0))
    items[total] = items[total - 1] | 3
    left[total] = 0
    pairs = (total + 1) >> 1

    def copy(i, ref, buf, sem, whole=False):
        entry = items[i]
        slot = i & (slots - 1)
        size = pl.multiple_of(jnp.where(whole, ITEM, sizes[i]), 16)
        return pltpu.make_async_copy(ref.at[first_seq + (entry >> 2), 0, pl.ds(pl.multiple_of((entry & 3) * ITEM, ITEM), size)], buf.at[slot, pl.ds(0, size)], sem.at[slot])

    def k_copy(i):
        return copy(i, key_ref, kbuf, k_sem)

    def v_copy(i):
        return copy(i, value_ref, vbuf, v_sem, i < slots)

    for i in range(slots - 2):
        @pl.when(i < total)
        def _():
            k_copy(i).start()
            v_copy(i).start()

    kn_out[...] = kn_ref[...]
    vn_out[...] = vn_ref[...]
    qs[...] = jnp.dot(perm[...], q_ref[...].reshape(768, 256), preferred_element_type=F32).astype(BF16)
    vnf[...] = vn_ref[pl.ds(pl.multiple_of(first_seq, 16), 16), :].astype(F32)
    knf = kn_ref[pl.ds(pl.multiple_of(first_seq, 16), 16), :].astype(F32)
    for n in range(16):
        rows = slice(n * 48, (n + 1) * 48)
        sn[rows] = jnp.broadcast_to(jnp.sum(qs[rows].astype(F32) * knf[n:n + 1], axis=1, keepdims=True), (48, 128))
    m_ref[...] = jnp.zeros_like(m_ref)
    l_ref[...] = jnp.ones_like(l_ref)
    acc[...] = jnp.zeros_like(acc)

    def rows_of(entry):
        return pl.ds(pl.multiple_of((entry >> 2) * 48, 16), 48)

    def score(i):
        return lax.dot_general(qs[rows_of(items[i]), :], kbuf[i & (slots - 1)], (((1,), (1,)), ((), ())), preferred_element_type=F32)

    lane = lax.broadcasted_iota(jnp.int32, (48, 128), 1)

    halves = (slice(0, 128), slice(128, 256))
    chunks = [slice(n * 128, (n + 1) * 128) for n in range(ITEM // 128)]

    def pair_scores(pair, turn):
        for n in range(2):
            sbuf[turn, n] = score(2 * pair + n)

    def weigh(pair, turn):
        m, l = m_ref[...], l_ref[...]
        for n in range(2):
            i = 2 * pair + n
            entry = items[i]
            fresh = (entry & 3) == 0
            m_old = jnp.where(fresh, sn[rows_of(entry), :], m)
            x = [jnp.where(lane < left[i] - c.start, sbuf[turn, n, :, c], -jnp.inf) for c in chunks]
            top = functools.reduce(jnp.maximum, x)
            m = jnp.maximum(m_old, jnp.broadcast_to(jnp.max(top, axis=1, keepdims=True), (48, 128)))
            alpha = jnp.exp2((m_old - m) * power)
            p = [jnp.exp2((v - m) * power) for v in x]
            l = jnp.where(fresh, 1.0, l) * alpha + jnp.broadcast_to(jnp.sum(functools.reduce(jnp.add, p), axis=1, keepdims=True), (48, 128))
            a_ref[turn, n] = alpha
            r_ref[turn, n] = l
            for c, v in zip(chunks, p):
                pbuf[turn, n, :, c] = v.astype(BF16)
        m_ref[...] = m
        l_ref[...] = l

    def blend(pair, turn):
        for n in range(2):
            i = 2 * pair + n
            entry = items[i]
            added = jnp.dot(pbuf[turn, n], vbuf[i & (slots - 1)], preferred_element_type=F32)
            alpha = a_ref[turn, n]
            inverse = 1.0 / r_ref[turn, n]
            fresh_row = vnf[pl.ds((entry >> 2), 1), :]
            for h in halves:
                now = jnp.where((entry & 3) == 0, jnp.broadcast_to(fresh_row[:, h], (48, 128)), acc[:, h]) * alpha + added[:, h]
                acc[:, h] = now
                os[rows_of(entry), h] = (now * inverse).astype(BF16)

    def arrive(copy, pair):
        for n in range(2):
            @pl.when(2 * pair + n < total)
            def _():
                copy(2 * pair + n).wait()

    arrive(k_copy, 0)
    pair_scores(0, 0)
    weigh(0, 0)
    arrive(k_copy, 1)
    pair_scores(jnp.minimum(1, pairs - 1), 1)

    @pl.loop(0, pairs)
    def _(pair):
        for n in range(2):
            i = 2 * pair + slots - 2 + n

            @pl.when(i < total)
            def _():
                k_copy(i).start()
                v_copy(i).start()

        arrive(k_copy, pair + 2)
        arrive(v_copy, pair)
        turn = pair & 1
        blend(pair, turn)
        weigh(jnp.minimum(pair + 1, pairs - 1), 1 - turn)
        pair_scores(jnp.minimum(pair + 2, pairs - 1), turn)

    mixed = jnp.dot(back[...], os[...], preferred_element_type=F32).astype(BF16)
    for h in range(48):
        o_ref[h // 6, :, (h % 6) * 256:(h % 6 + 1) * 256] = mixed[h * 16:(h + 1) * 16]


def attend(lengths, queries, key_new, value_new, perm, back, key_cache, value_cache):
    slots = 16
    vmem = pl.BlockSpec(memory_space=pltpu.VMEM)
    hbm = pl.BlockSpec(memory_space=pltpu.HBM)
    return pl.pallas_call(
        functools.partial(attend_kernel, slots),
        out_shape=(jax.ShapeDtypeStruct((8, 16, 1536), BF16), jax.ShapeDtypeStruct((32, 256), BF16), jax.ShapeDtypeStruct((32, 256), BF16)),
        in_specs=[pl.BlockSpec(memory_space=pltpu.SMEM), vmem, vmem, vmem, vmem, vmem, hbm, hbm],
        out_specs=(vmem, vmem, vmem),
        scratch_shapes=[
            pltpu.VMEM((slots, ITEM, 256), BF16),
            pltpu.VMEM((slots, ITEM, 256), BF16),
            pltpu.VMEM((768, 256), BF16),
            pltpu.VMEM((768, 256), BF16),
            pltpu.VMEM((768, 128), F32),
            pltpu.VMEM((16, 256), F32),
            pltpu.VMEM((2, 2, 48, ITEM), F32),
            pltpu.VMEM((2, 2, 48, ITEM), BF16),
            pltpu.VMEM((48, 256), F32),
            pltpu.VMEM((48, 128), F32),
            pltpu.VMEM((48, 128), F32),
            pltpu.VMEM((2, 2, 48, 128), F32),
            pltpu.VMEM((2, 2, 48, 128), F32),
            pltpu.SMEM((72,), jnp.int32),
            pltpu.SMEM((72,), jnp.int32),
            pltpu.SMEM((72,), jnp.int32),
            pltpu.SemaphoreType.DMA((slots,)),
            pltpu.SemaphoreType.DMA((slots,)),
        ],
        compiler_params=pltpu.CompilerParams(vmem_limit_bytes=40 * MIB),
        cost_estimate=pl.CostEstimate(flops=4 * 16 * 48 * 2048 * 256, bytes_accessed=16 * 2048 * 1024, transcendentals=16 * 48 * 2048),
        name="attend",
    )(lengths, queries, key_new, value_new, perm, back, key_cache, value_cache)


LAGS = (2, 5, 10, 14, 17)


def mix_kernel(chunk, slots, o_ref, w_ref, x_ref, out_ref, o_all, wbuf, xrows, part, r0, r1, r2,
               w_sem, x_sem, o_send, o_recv, o_self_sem, s0s, s1s, s2s, g1s, g2s, g3s, g3r, s0r, s1r, s2r, g1r, g2r):
    y, model, x, core = coordinates()
    me = y * 4 + model
    width = w_ref.shape[1]
    chunks = width // chunk
    first, second = x * (1 - core) + y * core, y * (1 - core) + x * core
    own = core * 4 + first * 2 + second
    flip_x = {"heads": y, "model": (1 - x) * 2 + core}
    partner = {"heads": y, "model": x * 2 + 1 - core}
    along_first = {"heads": y * (1 - core) + (1 - y) * core, "model": ((1 - x) * (1 - core) + x * core) * 2 + core}
    along_second = {"heads": (1 - y) * (1 - core) + y * core, "model": (x * (1 - core) + (1 - x) * core) * 2 + core}

    def w_copy(t):
        return pltpu.make_async_copy(w_ref.at[:, pl.ds(pl.multiple_of(t * chunk, chunk), chunk)], wbuf.at[t % slots], w_sem.at[t % slots])

    for t in range(slots):
        w_copy(t).start()
    x_copy = pltpu.make_async_copy(x_ref.at[pl.ds(own * 16, 16)], xrows, x_sem)
    x_copy.start()

    greet(range(1, 8))
    pl.semaphore_wait(pltpu.get_barrier_semaphore(), 7)

    mine = model * 2 + y

    def o_copy(offset):
        peer = (me + offset) % 8
        return pltpu.make_async_remote_copy(
            src_ref=o_ref.at[peer], dst_ref=o_all.at[pl.ds(mine * 16, 16)], send_sem=o_send, recv_sem=o_recv,
            device_id={"heads": peer // 4, "model": peer % 4}, device_id_type=MESH)

    for offset in range(1, 8):
        o_copy(offset).start()
    o_self = pltpu.make_async_copy(o_ref.at[me], o_all.at[pl.ds(mine * 16, 16)], o_self_sem)
    o_self.start()
    o_self.wait()
    pltpu.make_async_copy(o_all.at[pl.ds(0, 112)], o_all.at[pl.ds(0, 112)], o_recv).wait()
    x_copy.wait()

    def remote(src, dst, send, recv, device):
        return pltpu.make_async_remote_copy(src_ref=src, dst_ref=dst, send_sem=send, recv_sem=recv, device_id=device, device_id_type=MESH)

    half, quarter = core * 64, core * 64 + first * 32
    eighth = quarter + second * 16
    cols = lambda j: pl.ds(pl.multiple_of(j * chunk, chunk), chunk)

    def s0(j):
        return remote(part.at[j, pl.ds((1 - core) * 64, 64)], r0.at[j], s0s, s0r.at[j], partner)

    def s1(j):
        return remote(part.at[j, pl.ds(half + (1 - first) * 32, 32)], r1.at[j], s1s, s1r.at[j], along_first)

    def s2(j):
        return remote(part.at[j, pl.ds(quarter + (1 - second) * 16, 16)], r2.at[j], s2s, s2r.at[j], along_second)

    def g1(j):
        piece = out_ref.at[pl.ds(eighth, 16), cols(j)]
        return remote(piece, piece, g1s, g1r.at[j], along_second)

    def g2(j):
        piece = out_ref.at[pl.ds(quarter, 32), cols(j)]
        return remote(piece, piece, g2s, g2r.at[j], along_first)

    def g3(j):
        piece = out_ref.at[pl.ds(half, 64), cols(j)]
        return remote(piece, piece, g3s, g3r, partner)

    def arrived(ref, sem):
        pltpu.make_async_copy(ref, ref, sem).wait()

    def at(t, lag, body):
        j = t - lag

        @pl.when(jnp.logical_and(j >= 0, j < chunks))
        def _():
            body(j)

    def stage5(j):
        arrived(out_ref.at[pl.ds(core * 64 + (1 - first) * 32, 32), cols(j)], g2r.at[j])
        g3(j).start()

    def stage4(j):
        arrived(out_ref.at[pl.ds(quarter + (1 - second) * 16, 16), cols(j)], g1r.at[j])
        g2(j).start()

    def stage3(j):
        arrived(r2.at[j], s2r.at[j])
        total = part[j, pl.ds(pl.multiple_of(eighth, 16), 16)] + r2[j]
        out_ref[pl.ds(pl.multiple_of(eighth, 16), 16), cols(j)] = (xrows[:, cols(j)].astype(F32) + total).astype(BF16)
        g1(j).start()

    def stage2(j):
        arrived(r1.at[j], s1r.at[j])
        part[j, pl.ds(pl.multiple_of(quarter, 16), 32)] += r1[j]
        s2(j).start()

    def stage1(j):
        arrived(r0.at[j], s0r.at[j])
        part[j, pl.ds(pl.multiple_of(half, 16), 64)] += r0[j]
        s1(j).start()

    def stage0(j):
        w_copy(j).wait()
        part[j] = jnp.dot(o_all[...], wbuf[j % slots], preferred_element_type=F32)

        @pl.when(j + slots < chunks)
        def _():
            w_copy(j + slots).start()
        s0(j).start()

    @pl.loop(0, chunks + LAGS[-1])
    def _(t):
        at(t, 0, stage0)
        at(t, LAGS[0], stage1)
        at(t, LAGS[1], stage2)
        at(t, LAGS[2], stage3)
        at(t, LAGS[3], stage4)
        at(t, LAGS[4], stage5)

    arrived(o_ref.at[pl.ds(0, 7)], o_send)
    arrived(out_ref.at[pl.ds(0, 64)], g3r)
    for ref, sem in ((r0, s0s), (r1, s1s), (r2, s2s), (out_ref.at[pl.ds(0, 16)], g1s), (out_ref.at[pl.ds(0, 32)], g2s), (out_ref.at[pl.ds(0, 64)], g3s)):
        arrived(ref, sem)


def mix(attended, w_out, tokens):
    depth, width = w_out.shape
    chunk, slots = 1024, 4
    chunks = width // chunk
    vmem = pl.BlockSpec(memory_space=pltpu.VMEM)
    hbm = pl.BlockSpec(memory_space=pltpu.HBM)
    sems = pltpu.SemaphoreType.DMA((chunks,))
    return pl.pallas_call(
        functools.partial(mix_kernel, chunk, slots),
        out_shape=jax.ShapeDtypeStruct((128, width), BF16),
        in_specs=[vmem, hbm, hbm],
        out_specs=vmem,
        scratch_shapes=[
            pltpu.VMEM((128, depth), BF16),
            pltpu.VMEM((slots, depth, chunk), BF16),
            pltpu.VMEM((16, width), BF16),
            pltpu.VMEM((chunks, 128, chunk), F32),
            pltpu.VMEM((chunks, 64, chunk), F32),
            pltpu.VMEM((chunks, 32, chunk), F32),
            pltpu.VMEM((chunks, 16, chunk), F32),
            pltpu.SemaphoreType.DMA((slots,)),
        ] + [pltpu.SemaphoreType.DMA] * 11 + [sems] * 5,
        compiler_params=pltpu.CompilerParams(collective_id=1, has_side_effects=True, vmem_limit_bytes=42 * MIB),
        cost_estimate=pl.CostEstimate(flops=2 * 128 * depth * width, bytes_accessed=depth * width * 2, transcendentals=0),
        name="mix",
    )(attended, *(pltpu.with_memory_space_constraint(a, pltpu.HBM) for a in (w_out, tokens)))


def solution(mesh):
    def local_step(tokens, w_query, w_key, w_value, w_out, key_cache, value_cache, lengths):
        queries, key_new, value_new, perm, back = project_queries(tokens, w_query, w_key, w_value)
        attended, key_new, value_new = attend(lengths, queries, key_new, value_new, perm, back, key_cache, value_cache)
        out_tokens = mix(attended, w_out, tokens)
        return (out_tokens, key_new.reshape(32, 1, 256), value_new.reshape(32, 1, 256))

    cache_spec = P(("replica", "model"), None, None, None)
    new_spec = P(("replica", "model"), None, None)
    return jax.shard_map(
        local_step,
        mesh=mesh,
        in_specs=(P("replica", None), P(None, ("heads", "model")), P(None, None), P(None, None), P(("heads", "model"), None), cache_spec, cache_spec, P(("replica", "model"))),
        out_specs=(P("replica", None), new_spec, new_spec),
        check_vma=False,
    )
```

```python
import functools

import jax
import jax.numpy as jnp
from jax import lax
from jax.experimental import pallas as pl
from jax.experimental.pallas import tpu as pltpu
from jax.sharding import PartitionSpec as P

MESH = pl.DeviceIdType.MESH
F32 = jnp.float32
BF16 = jnp.bfloat16
MIB = 1 << 20


def coordinates():
    y = lax.axis_index("heads")
    model = lax.axis_index("model")
    return y, model, model // 2, model % 2


def greet(others):
    y, model, _, _ = coordinates()
    me = y * 4 + model
    barrier = pltpu.get_barrier_semaphore()
    for offset in others:
        peer = (me + offset) % 8
        pl.semaphore_signal(barrier, inc=1, device_id={"heads": peer // 4, "model": peer % 4}, device_id_type=MESH)


def query_kernel(groups, cols, depth, slots, kv_depth, x_ref, wq_ref, wk_ref, wv_ref, q_ref, kn_ref, vn_ref, perm, back, xbuf, wbuf, kvbuf, acc, kvacc, qs, kvs, kv_all,
                 x_sem, w_sem, kv_sem, q_send, q_recv, kv_send, kv_recv, self_sem, kv_self_sem):
    y, model, _, _ = coordinates()
    me = y * 4 + model
    width = x_ref.shape[1]
    steps = width // depth
    kv_steps = width // kv_depth
    total = groups * steps

    def w_copy(i):
        g, k = i // steps, i % steps
        return pltpu.make_async_copy(wq_ref.at[pl.ds(k * depth, depth), pl.ds(g * cols, cols)], wbuf.at[i % slots], w_sem.at[i % slots])

    def x_copy(k):
        part = pl.ds(pl.multiple_of(k * depth, 128), depth)
        return pltpu.make_async_copy(x_ref.at[:, part], xbuf.at[:, part], x_sem.at[k])

    def kv_copy(ref, col, k):
        return pltpu.make_async_copy(ref.at[pl.ds(k * kv_depth, kv_depth), pl.ds(col * 128, 128)], kvbuf.at[k], kv_sem.at[k])

    for i in range(max(steps, slots)):
        if i < steps:
            x_copy(i).start()
        if i < slots:
            w_copy(i).start()

    greet(range(1, 8))
    column = lax.broadcasted_iota(jnp.int32, (48, 768), 1)
    row = lax.broadcasted_iota(jnp.int32, (48, 768), 0)
    for n in range(16):
        perm[n * 48:(n + 1) * 48] = jnp.where(column == row * 16 + n, 1.0, 0.0).astype(BF16)
        back[n * 48:(n + 1) * 48] = jnp.where(column == row % 16 * 48 + row // 16 + 3 * n, 1.0, 0.0).astype(BF16)
    pl.semaphore_wait(pltpu.get_barrier_semaphore(), 7)

    per_group = cols // 256

    def q_copy(g, h, offset):
        head = g * per_group + h
        peer = (me + offset) % 8
        rows = (peer % 4) * 2 + peer // 4
        return pltpu.make_async_remote_copy(
            src_ref=qs.at[head, pl.ds(rows * 16, 16)], dst_ref=q_ref.at[me * 6 + head],
            send_sem=q_send, recv_sem=q_recv,
            device_id={"heads": peer // 4, "model": peer % 4}, device_id_type=MESH)

    def q_self(head):
        return pltpu.make_async_copy(qs.at[head, pl.ds((model * 2 + y) * 16, 16)], q_ref.at[me * 6 + head], self_sem)

    @pl.loop(0, total)
    def _(i):
        g, k = i // steps, i % steps

        @pl.when(i < steps)
        def _():
            x_copy(i).wait()

        w_copy(i).wait()
        part = jnp.dot(xbuf[:, pl.ds(pl.multiple_of(k * depth, 128), depth)], wbuf[i % slots], preferred_element_type=F32)

        @pl.when(k == 0)
        def _():
            acc[...] = part

        @pl.when(k > 0)
        def _():
            acc[...] += part

        @pl.when(i + slots < total)
        def _():
            w_copy(i + slots).start()

        for n in range(kv_steps):
            @pl.when(i == total - kv_steps + n - 1)
            def _():
                @pl.when(model < 2)
                def _():
                    kv_copy(wk_ref, model % 2, n).start()

                @pl.when(model >= 2)
                def _():
                    kv_copy(wv_ref, model % 2, n).start()

        @pl.when(k == steps - 1)
        def _():
            for h in range(per_group):
                qs[g * per_group + h] = acc[:, h * 256:(h + 1) * 256].astype(BF16)
            for h in range(per_group):
                for offset in (7, 6, 5, 4, 3, 2, 1):
                    q_copy(g, h, offset).start()
                q_self(g * per_group + h).start()

    kvacc[...] = jnp.zeros_like(kvacc)

    @pl.loop(0, kv_steps)
    def _(k):
        kv_copy(wk_ref, 0, k).wait()
        kvacc[...] += jnp.dot(xbuf[:, pl.ds(pl.multiple_of(k * kv_depth, 128), kv_depth)], kvbuf[k], preferred_element_type=F32)

    kvs[...] = kvacc[...].astype(BF16)

    def kv_send_copy(offset):
        peer = (model + offset) % 4
        return pltpu.make_async_remote_copy(
            src_ref=kvs.at[pl.ds(peer * 32, 32)], dst_ref=kv_all.at[model], send_sem=kv_send, recv_sem=kv_recv,
            device_id={"heads": y, "model": peer}, device_id_type=MESH)

    for offset in (2, 3, 1):
        kv_send_copy(offset).start()
    kv_self = pltpu.make_async_copy(kvs.at[pl.ds(model * 32, 32)], kv_all.at[model], kv_self_sem)
    kv_self.start()

    def settle(ref, sem):
        pltpu.make_async_copy(ref, ref, sem).wait()

    settle(q_ref.at[pl.ds(0, 6)], self_sem)
    settle(q_ref.at[pl.ds(0, 42)], q_send)
    settle(q_ref.at[pl.ds(0, 42)], q_recv)
    kv_self.wait()
    settle(kv_all.at[pl.ds(0, 3)], kv_send)
    settle(kv_all.at[pl.ds(0, 3)], kv_recv)
    kn_ref[:, :128] = kv_all[0]
    kn_ref[:, 128:] = kv_all[1]
    vn_ref[:, :128] = kv_all[2]
    vn_ref[:, 128:] = kv_all[3]


def project_queries(tokens, w_query, w_key, w_value):
    rows, width = tokens.shape
    groups, cols, depth, slots = 6, 256, 4608, 6
    kv_depth = 4608
    vmem = pl.BlockSpec(memory_space=pltpu.VMEM)
    hbm = pl.BlockSpec(memory_space=pltpu.HBM)
    return pl.pallas_call(
        functools.partial(query_kernel, groups, cols, depth, slots, kv_depth),
        out_shape=(jax.ShapeDtypeStruct((48, 16, 256), BF16), jax.ShapeDtypeStruct((32, 256), BF16), jax.ShapeDtypeStruct((32, 256), BF16),
                   jax.ShapeDtypeStruct((768, 768), BF16), jax.ShapeDtypeStruct((768, 768), BF16)),
        in_specs=[hbm, hbm, hbm, hbm],
        out_specs=(vmem,) * 5,
        scratch_shapes=[
            pltpu.VMEM((rows, width), BF16),
            pltpu.VMEM((slots, depth, cols), BF16),
            pltpu.VMEM((width // kv_depth, kv_depth, 128), BF16),
            pltpu.VMEM((rows, cols), F32),
            pltpu.VMEM((rows, 128), F32),
            pltpu.VMEM((6, rows, 256), BF16),
            pltpu.VMEM((rows, 128), BF16),
            pltpu.VMEM((4, 32, 128), BF16),
            pltpu.SemaphoreType.DMA((width // depth,)),
            pltpu.SemaphoreType.DMA((slots,)),
            pltpu.SemaphoreType.DMA((width // kv_depth,)),
        ] + [pltpu.SemaphoreType.DMA] * 6,
        compiler_params=pltpu.CompilerParams(collective_id=0, has_side_effects=True, vmem_limit_bytes=48 * MIB),
        cost_estimate=pl.CostEstimate(flops=2 * rows * width * 1664, bytes_accessed=width * 1664 * 2, transcendentals=0),
        name="query",
    )(*(pltpu.with_memory_space_constraint(a, pltpu.HBM) for a in (tokens, w_query, w_key, w_value)))


ITEM = 1024


def attend_kernel(slots, len_ref, q_ref, kn_ref, vn_ref, perm, back, key_ref, value_ref, o_ref, kn_out, vn_out, kbuf, vbuf, qs, os, sn, vnf, sbuf, pbuf, acc, m_ref, l_ref, a_ref, r_ref, items, left, sizes, k_sem, v_sem):
    y = lax.axis_index("heads")
    first_seq = y * 16
    power = 256 ** -0.5 * 1.4426950408889634

    def list_seq(s, count):
        length = len_ref[first_seq + s]
        chunks = (length + ITEM - 1) >> 10
        for c in range(4):
            @pl.when(c < chunks)
            def _():
                items[count + c] = s * 4 + c
                left[count + c] = length - c * ITEM
                sizes[count + c] = jnp.minimum((length - c * ITEM + 15) & ~15, ITEM)
        return count + chunks

    total = lax.fori_loop(0, 16, list_seq, jnp.int32(0))
    items[total] = items[total - 1] | 3
    left[total] = 0
    pairs = (total + 1) >> 1

    def copy(i, ref, buf, sem, whole=False):
        entry = items[i]
        slot = i & (slots - 1)
        size = pl.multiple_of(jnp.where(whole, ITEM, sizes[i]), 16)
        return pltpu.make_async_copy(ref.at[first_seq + (entry >> 2), 0, pl.ds(pl.multiple_of((entry & 3) * ITEM, ITEM), size)], buf.at[slot, pl.ds(0, size)], sem.at[slot])

    def k_copy(i):
        return copy(i, key_ref, kbuf, k_sem)

    def v_copy(i):
        return copy(i, value_ref, vbuf, v_sem, i < slots)

    for i in range(slots - 2):
        @pl.when(i < total)
        def _():
            k_copy(i).start()
            v_copy(i).start()

    kn_out[...] = kn_ref[...]
    vn_out[...] = vn_ref[...]
    qs[...] = jnp.dot(perm[...], q_ref[...].reshape(768, 256), preferred_element_type=F32).astype(BF16)
    vnf[...] = vn_ref[pl.ds(pl.multiple_of(first_seq, 16), 16), :].astype(F32)
    knf = kn_ref[pl.ds(pl.multiple_of(first_seq, 16), 16), :].astype(F32)
    for n in range(16):
        rows = slice(n * 48, (n + 1) * 48)
        sn[rows] = jnp.broadcast_to(jnp.sum(qs[rows].astype(F32) * knf[n:n + 1], axis=1, keepdims=True), (48, 128))
    m_ref[...] = jnp.zeros_like(m_ref)
    l_ref[...] = jnp.ones_like(l_ref)
    acc[...] = jnp.zeros_like(acc)

    def rows_of(entry):
        return pl.ds(pl.multiple_of((entry >> 2) * 48, 16), 48)

    def score(i):
        return lax.dot_general(qs[rows_of(items[i]), :], kbuf[i & (slots - 1)], (((1,), (1,)), ((), ())), preferred_element_type=F32)

    lane = lax.broadcasted_iota(jnp.int32, (48, 128), 1)

    halves = (slice(0, 128), slice(128, 256))
    chunks = [slice(n * 128, (n + 1) * 128) for n in range(ITEM // 128)]

    def pair_scores(pair, turn):
        for n in range(2):
            sbuf[turn, n] = score(2 * pair + n)

    def weigh(pair, turn):
        m, l = m_ref[...], l_ref[...]
        for n in range(2):
            i = 2 * pair + n
            entry = items[i]
            fresh = (entry & 3) == 0
            m_old = jnp.where(fresh, sn[rows_of(entry), :], m)
            x = [jnp.where(lane < left[i] - c.start, sbuf[turn, n, :, c], -jnp.inf) for c in chunks]
            top = functools.reduce(jnp.maximum, x)
            m = jnp.maximum(m_old, jnp.broadcast_to(jnp.max(top, axis=1, keepdims=True), (48, 128)))
            alpha = jnp.exp2((m_old - m) * power)
            p = [jnp.exp2((v - m) * power) for v in x]
            l = jnp.where(fresh, 1.0, l) * alpha + jnp.broadcast_to(jnp.sum(functools.reduce(jnp.add, p), axis=1, keepdims=True), (48, 128))
            a_ref[turn, n] = jnp.where(fresh, alpha.astype(BF16).astype(F32), alpha)
            r_ref[turn, n] = l
            for c, v in zip(chunks, p):
                pbuf[turn, n, :, c] = v.astype(BF16)
        m_ref[...] = m
        l_ref[...] = l

    def blend(pair, turn):
        for n in range(2):
            i = 2 * pair + n
            entry = items[i]
            added = jnp.dot(pbuf[turn, n], vbuf[i & (slots - 1)], preferred_element_type=F32)
            alpha = a_ref[turn, n]
            inverse = 1.0 / r_ref[turn, n]
            fresh_row = vnf[pl.ds((entry >> 2), 1), :]
            for h in halves:
                now = jnp.where((entry & 3) == 0, jnp.broadcast_to(fresh_row[:, h], (48, 128)), acc[:, h]) * alpha + added[:, h]
                acc[:, h] = now
                os[rows_of(entry), h] = (now * inverse).astype(BF16)

    def arrive(copy, pair):
        for n in range(2):
            @pl.when(2 * pair + n < total)
            def _():
                copy(2 * pair + n).wait()

    arrive(k_copy, 0)
    pair_scores(0, 0)
    weigh(0, 0)
    arrive(k_copy, 1)
    pair_scores(jnp.minimum(1, pairs - 1), 1)

    @pl.loop(0, pairs)
    def _(pair):
        for n in range(2):
            i = 2 * pair + slots - 2 + n

            @pl.when(i < total)
            def _():
                k_copy(i).start()
                v_copy(i).start()

        arrive(k_copy, pair + 2)
        arrive(v_copy, pair)
        turn = pair & 1
        blend(pair, turn)
        weigh(jnp.minimum(pair + 1, pairs - 1), 1 - turn)
        pair_scores(jnp.minimum(pair + 2, pairs - 1), turn)

    mixed = jnp.dot(back[...], os[...], preferred_element_type=F32).astype(BF16)
    for h in range(48):
        o_ref[h // 6, :, (h % 6) * 256:(h % 6 + 1) * 256] = mixed[h * 16:(h + 1) * 16]


def attend(lengths, queries, key_new, value_new, perm, back, key_cache, value_cache):
    slots = 16
    vmem = pl.BlockSpec(memory_space=pltpu.VMEM)
    hbm = pl.BlockSpec(memory_space=pltpu.HBM)
    return pl.pallas_call(
        functools.partial(attend_kernel, slots),
        out_shape=(jax.ShapeDtypeStruct((8, 16, 1536), BF16), jax.ShapeDtypeStruct((32, 256), BF16), jax.ShapeDtypeStruct((32, 256), BF16)),
        in_specs=[pl.BlockSpec(memory_space=pltpu.SMEM), vmem, vmem, vmem, vmem, vmem, hbm, hbm],
        out_specs=(vmem, vmem, vmem),
        scratch_shapes=[
            pltpu.VMEM((slots, ITEM, 256), BF16),
            pltpu.VMEM((slots, ITEM, 256), BF16),
            pltpu.VMEM((768, 256), BF16),
            pltpu.VMEM((768, 256), BF16),
            pltpu.VMEM((768, 128), F32),
            pltpu.VMEM((16, 256), F32),
            pltpu.VMEM((2, 2, 48, ITEM), F32),
            pltpu.VMEM((2, 2, 48, ITEM), BF16),
            pltpu.VMEM((48, 256), F32),
            pltpu.VMEM((48, 128), F32),
            pltpu.VMEM((48, 128), F32),
            pltpu.VMEM((2, 2, 48, 128), F32),
            pltpu.VMEM((2, 2, 48, 128), F32),
            pltpu.SMEM((72,), jnp.int32),
            pltpu.SMEM((72,), jnp.int32),
            pltpu.SMEM((72,), jnp.int32),
            pltpu.SemaphoreType.DMA((slots,)),
            pltpu.SemaphoreType.DMA((slots,)),
        ],
        compiler_params=pltpu.CompilerParams(vmem_limit_bytes=40 * MIB),
        cost_estimate=pl.CostEstimate(flops=4 * 16 * 48 * 2048 * 256, bytes_accessed=16 * 2048 * 1024, transcendentals=16 * 48 * 2048),
        name="attend",
    )(lengths, queries, key_new, value_new, perm, back, key_cache, value_cache)


LAGS = (2, 5, 10, 14, 17)


def mix_kernel(chunk, slots, o_ref, w_ref, x_ref, out_ref, o_all, wbuf, xrows, part, r0, r1, r2,
               w_sem, x_sem, o_send, o_recv, o_self_sem, s0s, s1s, s2s, g1s, g2s, g3s, g3r, s0r, s1r, s2r, g1r, g2r):
    y, model, x, core = coordinates()
    me = y * 4 + model
    width = w_ref.shape[1]
    chunks = width // chunk
    first, second = x * (1 - core) + y * core, y * (1 - core) + x * core
    own = core * 4 + first * 2 + second
    flip_x = {"heads": y, "model": (1 - x) * 2 + core}
    partner = {"heads": y, "model": x * 2 + 1 - core}
    along_first = {"heads": y * (1 - core) + (1 - y) * core, "model": ((1 - x) * (1 - core) + x * core) * 2 + core}
    along_second = {"heads": (1 - y) * (1 - core) + y * core, "model": (x * (1 - core) + (1 - x) * core) * 2 + core}

    def w_copy(t):
        return pltpu.make_async_copy(w_ref.at[:, pl.ds(pl.multiple_of(t * chunk, chunk), chunk)], wbuf.at[t % slots], w_sem.at[t % slots])

    for t in range(slots):
        w_copy(t).start()
    x_copy = pltpu.make_async_copy(x_ref.at[pl.ds(own * 16, 16)], xrows, x_sem)
    x_copy.start()

    greet(range(1, 8))
    pl.semaphore_wait(pltpu.get_barrier_semaphore(), 7)

    mine = model * 2 + y

    def o_copy(offset):
        peer = (me + offset) % 8
        return pltpu.make_async_remote_copy(
            src_ref=o_ref.at[peer], dst_ref=o_all.at[pl.ds(mine * 16, 16)], send_sem=o_send, recv_sem=o_recv,
            device_id={"heads": peer // 4, "model": peer % 4}, device_id_type=MESH)

    for offset in range(1, 8):
        o_copy(offset).start()
    o_self = pltpu.make_async_copy(o_ref.at[me], o_all.at[pl.ds(mine * 16, 16)], o_self_sem)
    o_self.start()
    o_self.wait()
    pltpu.make_async_copy(o_all.at[pl.ds(0, 112)], o_all.at[pl.ds(0, 112)], o_recv).wait()
    x_copy.wait()

    def remote(src, dst, send, recv, device):
        return pltpu.make_async_remote_copy(src_ref=src, dst_ref=dst, send_sem=send, recv_sem=recv, device_id=device, device_id_type=MESH)

    half, quarter = core * 64, core * 64 + first * 32
    eighth = quarter + second * 16
    cols = lambda j: pl.ds(pl.multiple_of(j * chunk, chunk), chunk)

    def s0(j):
        return remote(part.at[j, pl.ds((1 - core) * 64, 64)], r0.at[j], s0s, s0r.at[j], partner)

    def s1(j):
        return remote(part.at[j, pl.ds(half + (1 - first) * 32, 32)], r1.at[j], s1s, s1r.at[j], along_first)

    def s2(j):
        return remote(part.at[j, pl.ds(quarter + (1 - second) * 16, 16)], r2.at[j], s2s, s2r.at[j], along_second)

    def g1(j):
        piece = out_ref.at[pl.ds(eighth, 16), cols(j)]
        return remote(piece, piece, g1s, g1r.at[j], along_second)

    def g2(j):
        piece = out_ref.at[pl.ds(quarter, 32), cols(j)]
        return remote(piece, piece, g2s, g2r.at[j], along_first)

    def g3(j):
        piece = out_ref.at[pl.ds(half, 64), cols(j)]
        return remote(piece, piece, g3s, g3r, partner)

    def arrived(ref, sem):
        pltpu.make_async_copy(ref, ref, sem).wait()

    def at(t, lag, body):
        j = t - lag

        @pl.when(jnp.logical_and(j >= 0, j < chunks))
        def _():
            body(j)

    def stage5(j):
        arrived(out_ref.at[pl.ds(core * 64 + (1 - first) * 32, 32), cols(j)], g2r.at[j])
        g3(j).start()

    def stage4(j):
        arrived(out_ref.at[pl.ds(quarter + (1 - second) * 16, 16), cols(j)], g1r.at[j])
        g2(j).start()

    def stage3(j):
        arrived(r2.at[j], s2r.at[j])
        total = part[j, pl.ds(pl.multiple_of(eighth, 16), 16)] + r2[j]
        out_ref[pl.ds(pl.multiple_of(eighth, 16), 16), cols(j)] = (xrows[:, cols(j)].astype(F32) + total).astype(BF16)
        g1(j).start()

    def stage2(j):
        arrived(r1.at[j], s1r.at[j])
        part[j, pl.ds(pl.multiple_of(quarter, 16), 32)] += r1[j]
        s2(j).start()

    def stage1(j):
        arrived(r0.at[j], s0r.at[j])
        part[j, pl.ds(pl.multiple_of(half, 16), 64)] += r0[j]
        s1(j).start()

    def stage0(j):
        w_copy(j).wait()
        part[j] = jnp.dot(o_all[...], wbuf[j % slots], preferred_element_type=F32)

        @pl.when(j + slots < chunks)
        def _():
            w_copy(j + slots).start()
        s0(j).start()

    @pl.loop(0, chunks + LAGS[-1])
    def _(t):
        at(t, 0, stage0)
        at(t, LAGS[0], stage1)
        at(t, LAGS[1], stage2)
        at(t, LAGS[2], stage3)
        at(t, LAGS[3], stage4)
        at(t, LAGS[4], stage5)

    arrived(o_ref.at[pl.ds(0, 7)], o_send)
    arrived(out_ref.at[pl.ds(0, 64)], g3r)
    for ref, sem in ((r0, s0s), (r1, s1s), (r2, s2s), (out_ref.at[pl.ds(0, 16)], g1s), (out_ref.at[pl.ds(0, 32)], g2s), (out_ref.at[pl.ds(0, 64)], g3s)):
        arrived(ref, sem)


def mix(attended, w_out, tokens):
    depth, width = w_out.shape
    chunk, slots = 1024, 4
    chunks = width // chunk
    vmem = pl.BlockSpec(memory_space=pltpu.VMEM)
    hbm = pl.BlockSpec(memory_space=pltpu.HBM)
    sems = pltpu.SemaphoreType.DMA((chunks,))
    return pl.pallas_call(
        functools.partial(mix_kernel, chunk, slots),
        out_shape=jax.ShapeDtypeStruct((128, width), BF16),
        in_specs=[vmem, hbm, hbm],
        out_specs=vmem,
        scratch_shapes=[
            pltpu.VMEM((128, depth), BF16),
            pltpu.VMEM((slots, depth, chunk), BF16),
            pltpu.VMEM((16, width), BF16),
            pltpu.VMEM((chunks, 128, chunk), F32),
            pltpu.VMEM((chunks, 64, chunk), F32),
            pltpu.VMEM((chunks, 32, chunk), F32),
            pltpu.VMEM((chunks, 16, chunk), F32),
            pltpu.SemaphoreType.DMA((slots,)),
        ] + [pltpu.SemaphoreType.DMA] * 11 + [sems] * 5,
        compiler_params=pltpu.CompilerParams(collective_id=1, has_side_effects=True, vmem_limit_bytes=42 * MIB),
        cost_estimate=pl.CostEstimate(flops=2 * 128 * depth * width, bytes_accessed=depth * width * 2, transcendentals=0),
        name="mix",
    )(attended, *(pltpu.with_memory_space_constraint(a, pltpu.HBM) for a in (w_out, tokens)))


def solution(mesh):
    def local_step(tokens, w_query, w_key, w_value, w_out, key_cache, value_cache, lengths):
        queries, key_new, value_new, perm, back = project_queries(tokens, w_query, w_key, w_value)
        attended, key_new, value_new = attend(lengths, queries, key_new, value_new, perm, back, key_cache, value_cache)
        out_tokens = mix(attended, w_out, tokens)
        return (out_tokens, key_new.reshape(32, 1, 256), value_new.reshape(32, 1, 256))

    cache_spec = P(("replica", "model"), None, None, None)
    new_spec = P(("replica", "model"), None, None)
    return jax.shard_map(
        local_step,
        mesh=mesh,
        in_specs=(P("replica", None), P(None, ("heads", "model")), P(None, None), P(None, None), P(("heads", "model"), None), cache_spec, cache_spec, P(("replica", "model"))),
        out_specs=(P("replica", None), new_spec, new_spec),
        check_vma=False,
    )
```
